512 devices in a mesh: dp: 8 (over y_hi, x), expert: 64 (over z, y_lo, core).
Axes of the slice: x: 4, y: 4 (y_hi: 2, y_lo: 2; y = y_hi * 2 + y_lo), z: 16, core: 2. Of those that a mesh axis runs over, the one named last changes fastest.
Arguments:
- tokens: bfloat16 [65536, 2048], P(('dp', 'expert')), may hold values from -6 to 6
- cotangent: bfloat16 [65536, 2048], P(('dp', 'expert')), may hold values from -6 to 6
- expert_ids: int32 [65536, 8], P(('dp', 'expert')), may hold values from 0 to 127, as said below
- gate_probs: float32 [65536, 8], P(('dp', 'expert')), may hold values from 0.1 to 1
- gate_weight: bfloat16 [64, 2048, 128], P('expert'), may hold values from -0.125 to 0.125
- up_weight: bfloat16 [64, 2048, 128], P('expert'), may hold values from -0.125 to 0.125
- down_weight: bfloat16 [64, 128, 2048], P('expert'), may hold values from -0.1875 to 0.1875
Outputs:
- grad_input: bfloat16 [65536, 2048], P(('dp', 'expert'))
- grad_gate: bfloat16 [64, 2048, 128], P('expert')
- grad_up: bfloat16 [64, 2048, 128], P('expert')
- grad_down: bfloat16 [64, 128, 2048], P('expert')
The draws below stay inside these ranges and needn't reach their ends.
Inputs may be any that keep to these rules, and one draw needn't show every extreme that they name: `expert_ids`: each row names 8 different experts. Among the 128 rows of one device, each window expert 0 to 7 is named by 1 to 8 rows, and in every draw one window expert of every device is named by exactly 8 rows.
All inputs are finite; a program needn't handle non-finite values.
Results may differ from the reference program's by a relative error of at most 0.0064.
Values may be sent and summed in bfloat16 or wider, within the bound.
A program may use at most 64 MiB of HBM per device.

```python
import math
import jax
import jax.numpy as jnp
from jax import lax

D = 2048
HID = 1024
EXPERTS = 128
TOP = 8
SLICES = 8
TOK_DEV = 128
CAP = 8
HSL = 128
EXP_WIN = 8
TOKENS = 65536


def draw_expert_ids(key, part):
    blocks = TOKENS // TOK_DEV
    window = EXP_WIN
    others = EXPERTS - window
    key_count, key_full, key_member, key_other, key_order = jax.random.split(jax.random.fold_in(key, 17), 5)
    counts = jax.random.randint(key_count, (blocks, window), 1, CAP + 1)
    full_one = jax.random.randint(key_full, (blocks,), 0, window)
    counts = jnp.where(jnp.arange(window)[None, :] == full_one[:, None], CAP, counts)
    member_score = jax.random.randint(key_member, (blocks, window, TOK_DEV), 0, 1 << 20) * TOK_DEV + jnp.arange(TOK_DEV)
    ordering = jnp.argsort(member_score, axis=-1)
    ranking = jnp.argsort(ordering, axis=-1)
    member = jnp.transpose(ranking < counts[:, :, None], (0, 2, 1)).astype(jnp.int32)
    window_key = (1 - member) * window + jnp.arange(window)
    window_sorted = jnp.argsort(window_key, axis=-1)
    window_count = jnp.sum(member, axis=-1)
    other_score = jax.random.randint(key_other, (blocks, TOK_DEV, others), 0, 1 << 20) * others + jnp.arange(others)
    unused, other_top = lax.top_k(other_score, TOP)
    other_ids = other_top + window
    position = jnp.arange(TOP)[None, None, :]
    window_pick = jnp.take_along_axis(window_sorted, jnp.broadcast_to(jnp.minimum(position, window - 1), (blocks, TOK_DEV, TOP)), axis=-1)
    other_index = jnp.clip(position - window_count[..., None], 0, TOP - 1)
    other_pick = jnp.take_along_axis(other_ids, other_index, axis=-1)
    combined = jnp.where(position < window_count[..., None], window_pick, other_pick)
    shuffle_score = jax.random.randint(key_order, (blocks, TOK_DEV, TOP), 0, 1 << 20) * TOP + position
    shuffle = jnp.argsort(shuffle_score, axis=-1)
    combined = jnp.take_along_axis(combined, shuffle, axis=-1)
    return combined.reshape(TOKENS, TOP).astype(jnp.int32)


def levels(rng, extent, cuts, low, high):
    gain = 1.0
    for dim, shards_of in cuts:
        draws = jax.random.uniform(jax.random.fold_in(jax.random.fold_in(rng, 6), dim), (shards_of,), jnp.float32, low / len(cuts), high / len(cuts))
        gain = gain * jnp.repeat(jnp.exp(draws), extent[dim] // shards_of).reshape((-1,) + (1,) * (len(extent) - 1 - dim))
    return gain


def gaussian(rng, dims, spread, reach, shards=(), kind=jnp.bfloat16):
    loudness = levels(rng, dims, shards, -0.22, 0.18) if shards else 1.0
    entries = jax.random.normal(rng, dims, jnp.float32) * spread * loudness
    return jnp.minimum(jnp.maximum(entries, -reach), reach).astype(kind)


def setup_inputs(seed: int = 0) -> dict:
    splits = jax.random.split(jax.random.key(seed), 8)
    return {
        "tokens": gaussian(splits[0], (TOKENS, D), 1.0, 6.0, ((0, 512),)),
        "cotangent": gaussian(splits[1], (TOKENS, D), 1.0, 6.0, ((0, 512),)),
        "expert_ids": draw_expert_ids(jax.random.fold_in(splits[7], 71), 0),
        "gate_probs": jnp.clip(jnp.exp(math.log(1.0) - 2.3025851 * jax.random.uniform(splits[3], (TOKENS, TOP), jnp.float32) ** levels(splits[3], (TOKENS, TOP), ((0, 512),), -0.2, 0.2)), 0.1, 1.0),
        "gate_weight": gaussian(splits[4], (SLICES * EXP_WIN, D, HSL), D ** -0.5, 0.125, ((0, 64),)),
        "up_weight": gaussian(splits[5], (SLICES * EXP_WIN, D, HSL), D ** -0.5, 0.125, ((0, 64),)),
        "down_weight": gaussian(splits[6], (SLICES * EXP_WIN, HSL, D), HID ** -0.5, 0.1875, ((0, 64),)),
    }


def silu_parts(gate_pre):
    sigmoid_value = jax.nn.sigmoid(gate_pre)
    return gate_pre * sigmoid_value, sigmoid_value * (1.0 + gate_pre * (1.0 - sigmoid_value))


def expert_slice(rows_in, rows_cot, gate_rows, up_rows, down_rows):
    gate_pre = jnp.dot(rows_in, gate_rows, preferred_element_type=jnp.float32)
    upward = jnp.dot(rows_in, up_rows, preferred_element_type=jnp.float32)
    swish, slope = silu_parts(gate_pre)
    active = (swish * upward).astype(jnp.bfloat16)
    dhidden = lax.dot_general(rows_cot, down_rows, (((1,), (1,)), ((), ())), preferred_element_type=jnp.float32)
    dgate = (dhidden * upward * slope).astype(jnp.bfloat16)
    dupward = (dhidden * swish).astype(jnp.bfloat16)
    grad_down = lax.dot_general(active, rows_cot, (((0,), (0,)), ((), ())), preferred_element_type=jnp.float32)
    grad_gate = lax.dot_general(rows_in, dgate, (((0,), (0,)), ((), ())), preferred_element_type=jnp.float32)
    grad_up = lax.dot_general(rows_in, dupward, (((0,), (0,)), ((), ())), preferred_element_type=jnp.float32)
    partial_value = lax.dot_general(dgate, gate_rows, (((1,), (1,)), ((), ())), preferred_element_type=jnp.float32)
    partial_value = partial_value + lax.dot_general(dupward, up_rows, (((1,), (1,)), ((), ())), preferred_element_type=jnp.float32)
    return partial_value, grad_gate, grad_up, grad_down


def reference(tokens, cotangent, expert_ids, gate_probs, gate_weight, up_weight, down_weight):
    blocks = TOKENS // TOK_DEV
    window = EXP_WIN
    id_blocks = expert_ids.reshape(blocks, TOK_DEV, TOP)
    prob_blocks = gate_probs.reshape(blocks, TOK_DEV, TOP)
    matched = id_blocks[..., None] == jnp.arange(window, dtype=jnp.int32)
    hit_count = jnp.sum(matched.astype(jnp.int32), axis=2)
    chosen = jnp.sum(jnp.where(matched, prob_blocks[..., None], jnp.float32(0)), axis=2)
    slot_rank = jnp.cumsum(hit_count, axis=1) - hit_count
    placed = (hit_count[..., None] == 1) & (slot_rank[..., None] == jnp.arange(CAP, dtype=jnp.int32))
    filled = jnp.any(placed, axis=1)
    positions = jnp.arange(TOK_DEV, dtype=jnp.int32)[None, :, None, None]
    owner_row = jnp.sum(jnp.where(placed, positions, 0), axis=1).astype(jnp.int32)
    block_index = jnp.arange(blocks, dtype=jnp.int32)[:, None, None]
    tok_blocks = tokens.reshape(blocks, TOK_DEV, D)
    cot_blocks = cotangent.reshape(blocks, TOK_DEV, D)
    rows_in = jnp.where(filled[..., None], tok_blocks[block_index, owner_row], jnp.zeros((), tokens.dtype))
    slot_prob = jnp.take_along_axis(jnp.transpose(chosen, (0, 2, 1)), owner_row, axis=2)
    scaled = slot_prob[..., None] * cot_blocks[block_index, owner_row].astype(jnp.float32)
    rows_cot = jnp.where(filled[..., None], scaled, jnp.float32(0)).astype(jnp.bfloat16)
    gate_list = []
    up_list = []
    down_list = []
    back_list = [jnp.zeros((blocks * CAP, D), jnp.float32) for expert_index in range(window)]
    for slice_index in range(SLICES):
        for expert_index in range(window):
            weight_row = slice_index * window + expert_index
            expert_in = rows_in[:, expert_index].reshape(blocks * CAP, D)
            expert_cot = rows_cot[:, expert_index].reshape(blocks * CAP, D)
            partial_value, grad_g, grad_u, grad_d = expert_slice(expert_in, expert_cot, gate_weight[weight_row], up_weight[weight_row], down_weight[weight_row])
            rounded = lax.optimization_barrier(partial_value.astype(jnp.bfloat16)).astype(jnp.float32)
            back_list[expert_index] = back_list[expert_index] + rounded
            gate_list.append(grad_g.astype(jnp.bfloat16))
            up_list.append(grad_u.astype(jnp.bfloat16))
            down_list.append(grad_d.astype(jnp.bfloat16))
    back_all = jnp.stack([item.reshape(blocks, CAP, D) for item in back_list], axis=1)
    grad_blocks = jnp.zeros((blocks, TOK_DEV, D), jnp.float32)
    grad_blocks = grad_blocks.at[block_index, owner_row].add(jnp.where(filled[..., None], back_all, jnp.float32(0)))
    grad_input = grad_blocks.reshape(TOKENS, D).astype(jnp.bfloat16)
    return grad_input, jnp.stack(gate_list), jnp.stack(up_list), jnp.stack(down_list)
```

```python
import jax
import jax.numpy as jnp
from jax import lax
from jax.sharding import PartitionSpec as P

SLICES = 8
CAP = 8
BF = jnp.bfloat16
F32 = jnp.float32


def local(tokens, cotangent, expert_ids, gate_probs, gate_weight, up_weight, down_weight):
    devices = lax.axis_size("expert")
    window = devices // SLICES
    cell = [[s * window + e for e in range(window)] for s in range(SLICES)]
    column = [[s * window + e for s in range(SLICES)] for e in range(window)]
    dp = lax.axis_size("dp")
    me = lax.axis_index("dp")
    width = tokens.shape[1]
    rows = tokens.shape[0]
    hid = down_weight.shape[1]
    piece = hid // dp
    gate_piece = lax.dynamic_slice(gate_weight[0], (0, me * piece), (width, piece)).T
    up_piece = lax.dynamic_slice(up_weight[0], (0, me * piece), (width, piece)).T
    down_piece = lax.dynamic_slice(down_weight[0], (me * piece, 0), (piece, width))
    weights = jnp.stack([gate_piece, up_piece, down_piece])
    weights = lax.all_gather(weights, "expert", axis=1, axis_index_groups=column)
    weights = weights.reshape(3 * hid, width)

    matched = expert_ids[:, :, None] == jnp.arange(window, dtype=jnp.int32)[None, None, :]
    hit = jnp.sum(matched.astype(jnp.int32), axis=1)
    chosen = jnp.sum(jnp.where(matched, gate_probs[:, :, None], 0.0), axis=1)
    rank = jnp.cumsum(hit, axis=0) - hit
    placed = (hit[:, :, None] == 1) & (
        rank[:, :, None] == jnp.arange(CAP, dtype=jnp.int32)[None, None, :]
    )
    picker = placed.astype(BF)
    slot_prob = jnp.sum(jnp.where(placed, chosen[:, :, None], 0.0), axis=0)
    rows_in = jnp.einsum("tec,td->ecd", picker, tokens, preferred_element_type=F32).astype(BF)
    picked = jnp.einsum("tec,td->ecd", picker, cotangent, preferred_element_type=F32)
    rows_cot = (slot_prob[:, :, None] * picked).astype(BF)
    message = jnp.concatenate([rows_in, rows_cot], axis=1)
    message = lax.all_to_all(
        message, "expert", split_axis=0, concat_axis=0, axis_index_groups=cell, tiled=True
    )
    both = lax.all_gather(message, "dp", axis=0)
    blocks = dp * window
    both = both.reshape(blocks * 2 * CAP, width)

    first = lax.dot_general(both, weights, (((1,), (1,)), ((), ())), preferred_element_type=F32)
    first = first.reshape(blocks, 2, CAP, 3, hid)
    pre = first[:, 0, :, 0]
    upward = first[:, 0, :, 1]
    dhidden = first[:, 1, :, 2]
    sigmoid = jax.nn.sigmoid(pre)
    swish = pre * sigmoid
    slope = sigmoid * (1.0 + pre * (1.0 - sigmoid))
    active = (swish * upward).astype(BF)
    dgate = (dhidden * upward * slope).astype(BF)
    dupward = (dhidden * swish).astype(BF)
    zero = jnp.zeros_like(active)
    left = jnp.concatenate(
        [
            jnp.concatenate([dgate, dupward, zero], axis=2),
            jnp.concatenate([zero, zero, active], axis=2),
        ],
        axis=1,
    ).reshape(blocks * 2 * CAP, 3 * hid)
    grads = lax.dot_general(left, both, (((0,), (0,)), ((), ())), preferred_element_type=F32)
    pair = jnp.concatenate([dgate, dupward], axis=2).reshape(blocks * CAP, 2 * hid)
    part = jnp.dot(pair, weights[: 2 * hid], preferred_element_type=F32).astype(BF)

    grads = grads.astype(BF).reshape(3, SLICES, piece, width).transpose(1, 0, 2, 3)
    grads = lax.psum_scatter(
        grads.reshape(SLICES * 3 * piece, width),
        "expert",
        scatter_dimension=0,
        axis_index_groups=column,
        tiled=True,
    ).reshape(3, piece, width)
    grads = lax.all_gather(grads, "dp", axis=1).reshape(3, hid, width)

    part = part.reshape(dp, window, CAP, width)
    part = lax.psum_scatter(part, "dp", scatter_dimension=0, tiled=False)
    back = lax.all_to_all(
        part, "expert", split_axis=0, concat_axis=0, axis_index_groups=cell, tiled=True
    )
    grad_input = lax.dot_general(
        picker.reshape(rows, window * CAP),
        back.reshape(window * CAP, width),
        (((1,), (0,)), ((), ())),
        preferred_element_type=F32,
    ).astype(BF)
    return (grad_input, grads[0].T[None], grads[1].T[None], grads[2][None])


def solution(mesh):
    tok = P(("dp", "expert"), None)
    wgt = P("expert", None, None)
    return jax.shard_map(
        local,
        mesh=mesh,
        in_specs=(tok, tok, tok, tok, wgt, wgt, wgt),
        out_specs=(tok, wgt, wgt, wgt),
        check_vma=False,
    )
```

```python
import jax
import jax.numpy as jnp
from jax import lax
from jax.experimental import pallas as pl
from jax.experimental.pallas import tpu as pltpu
from jax.sharding import PartitionSpec as P

SLICES = 8
CAP = 8
XS = 4
BF = jnp.bfloat16
F32 = jnp.float32
MESH = pl.DeviceIdType.MESH
DMA = pltpu.SemaphoreType.DMA
FLIPS = [(fz, fy, fc) for fz in (0, 1) for fy in (0, 1) for fc in (0, 1)]


def kernel(
    ids_ref,
    probs_ref,
    tok_hbm,
    cot_hbm,
    gate_hbm,
    up_hbm,
    down_hbm,
    gi_ref,
    fg,
    tok,
    cot,
    gate,
    up,
    down,
    msg,
    x_all,
    w_all,
    lt,
    pair,
    grad,
    part,
    zs,
    zr,
    ps0,
    pr0,
    ps1,
    pr1,
    ys,
    yr,
    bs,
    br,
    load_sem,
    za_s,
    za_r,
    ca_s,
    ca_r,
    ya_s,
    ya_r,
    xa_s,
    xa_r,
    xb_s,
    xb_r,
    zg_s,
    zg_r,
    p0_s,
    p0_r,
    p1_s,
    p1_r,
    yb_s,
    yb_r,
    cb_s,
    cb_r,
    yg_s,
    yg_r,
    xg_s,
    xg_r,
    xh_s,
    xh_r,
):
    width = tok.shape[1]
    half = width // 2
    dp = lax.axis_index("dp")
    ex = lax.axis_index("expert")
    s = ex // 8
    e = ex % 8
    zb, yl, co = e // 4, (e // 2) % 2, e % 2
    x, yh = dp % XS, dp // XS
    oyh = 1 - yh

    def ring(k):
        return (s + k + 8) % 8

    def flip(f):
        fz, fy, fc = f
        return ((zb + fz) % 2) * 4 + ((yl + fy) % 2) * 2 + (co + fc) % 2

    def group(j):
        return ((zb + j // 2) % 2) * 2 + (yl + j % 2) % 2

    def dpx(rel, k):
        return (oyh if rel else yh) * XS + (x + k + XS) % XS

    z_to = [(dp, ring(1) * 8 + e), (dp, ring(-1) * 8 + e)]
    x_to = [(dpx(0, 1), ex), (dpx(0, -1), ex)]
    y_to = (dpx(1, 0), ex)
    c_to = [(dp, s * 8 + flip(f)) for f in FLIPS]
    sends = []

    def send(src, dst, ssem, rsem, to):
        c = pltpu.make_async_remote_copy(
            src_ref=src, dst_ref=dst, send_sem=ssem, recv_sem=rsem, device_id=to, device_id_type=MESH
        )
        c.start()
        sends.append(c)

    def arrive(dst, ssem, rsem, frm):
        pltpu.make_async_remote_copy(
            src_ref=dst, dst_ref=dst, send_sem=ssem, recv_sem=rsem, device_id=frm, device_id_type=MESH
        ).wait_recv()

    loads = [
        pltpu.make_async_copy(a, b, load_sem.at[i])
        for i, (a, b) in enumerate(
            [(gate_hbm.at[0], gate), (up_hbm.at[0], up), (down_hbm.at[0], down), (tok_hbm, tok), (cot_hbm, cot)]
        )
    ]
    for c in loads:
        c.start()

    barrier = pltpu.get_barrier_semaphore()
    partners = z_to + x_to + [y_to] + c_to[1:]
    for to in partners:
        pl.semaphore_signal(barrier, inc=1, device_id=to, device_id_type=MESH)

    row = lax.broadcasted_iota(jnp.int32, (16, 128), 0)
    lane = lax.broadcasted_iota(jnp.int32, (16, 128), 1)
    sel = jnp.where(lane == row + dp * 16, 1.0, 0.0).astype(BF)
    loads[0].wait()
    w_all[0, s] = lax.dot_general(
        sel, gate[...], (((1,), (1,)), ((), ())), preferred_element_type=F32
    ).astype(BF)
    loads[1].wait()
    w_all[1, s] = lax.dot_general(
        sel, up[...], (((1,), (1,)), ((), ())), preferred_element_type=F32
    ).astype(BF)
    loads[2].wait()
    w_all[2, s] = down[pl.ds(pl.multiple_of(dp * 16, 16), 16), :]
    pl.semaphore_wait(barrier, len(partners))

    def w_send(dr, k, t):
        c = ring(-k if dr == 0 else k)
        ref = w_all.at[t, c] if k < 3 else w_all.at[t, c, :, pl.ds(dr * half, half)]
        send(ref, ref, za_s.at[dr, k, t], za_r.at[dr, k, t], z_to[dr])

    def w_arrive(k, t):
        for dr in (0, 1):
            c = ring(-1 - k if dr == 0 else 1 + k)
            ref = w_all.at[t, c] if k < 3 else w_all.at[t, c, :, pl.ds(dr * half, half)]
            arrive(ref, za_s.at[dr, k, t], za_r.at[dr, k, t], z_to[1 - dr])
            if k < 3:
                w_send(dr, k + 1, t)

    for dr in (0, 1):
        w_send(dr, 0, 0)

    ids = ids_ref[...]
    probs = probs_ref[...]
    want = lax.broadcasted_iota(jnp.int32, (128, 128), 1) // CAP
    slot = (lax.broadcasted_iota(jnp.int32, (128, 128), 1) % CAP).astype(F32)
    hit = jnp.zeros((128, 128), F32)
    chosen = jnp.zeros((128, 128), F32)
    for k in range(ids.shape[1]):
        m = ids[:, k : k + 1] == want
        hit = hit + jnp.where(m, 1.0, 0.0)
        chosen = chosen + jnp.where(m, probs[:, k : k + 1], 0.0)
    below = jnp.where(
        lax.broadcasted_iota(jnp.int32, (128, 128), 1) < lax.broadcasted_iota(jnp.int32, (128, 128), 0),
        1.0,
        0.0,
    ).astype(BF)
    rank = jnp.dot(below, hit.astype(BF), preferred_element_type=F32)
    placed = jnp.where((hit == 1.0) & (rank == slot) & (want < 8), 1.0, 0.0)
    picker_t = placed.T[:64].astype(BF)
    prob_t = jnp.sum((placed * chosen).T[:64], axis=1, keepdims=True)
    loads[3].wait()
    rows_in = jnp.dot(picker_t, tok[...], preferred_element_type=F32)
    loads[4].wait()
    rows_cot = prob_t * jnp.dot(picker_t, cot[...], preferred_element_type=F32)
    msg[...] = jnp.concatenate(
        [rows_in.reshape(8, CAP, width), rows_cot.reshape(8, CAP, width)], axis=1
    ).astype(BF)
    for i in range(1, 8):
        send(msg.at[flip(FLIPS[i])], x_all.at[dp, e], ca_s.at[i], ca_r.at[i], c_to[i])
    x_all[dp, e] = msg[e]
    for t in (1, 2):
        for dr in (0, 1):
            w_send(dr, 0, t)

    def grp(d, j):
        return x_all.at[d, pl.ds(group(j) * 2, 2)]

    def xa_send(rel, j):
        for dr in (0, 1):
            ref = grp(dpx(rel, 0), j)
            send(ref, ref, xa_s.at[dr, rel, j], xa_r.at[dr, rel, j], x_to[dr])

    def cell_group(j):
        for fc in (0, 1):
            i = j * 2 + fc
            if i:
                ref = x_all.at[dp, flip(FLIPS[i])]
                arrive(ref, ca_s.at[i], ca_r.at[i], c_to[i])
        xa_send(0, j)
        ref = grp(dp, j)
        send(ref, ref, ya_s.at[j], ya_r.at[j], y_to)

    def y_group(j):
        arrive(grp(dpx(1, 0), j), ya_s.at[j], ya_r.at[j], y_to)
        xa_send(1, j)

    def xa_arrive(dr, rel, j):
        arrive(grp(dpx(rel, -1 if dr == 0 else 1), j), xa_s.at[dr, rel, j], xa_r.at[dr, rel, j], x_to[1 - dr])

    def relay(rel, j):
        dr = j // 2
        xa_arrive(dr, rel, j)
        ref = grp(dpx(rel, -1 if dr == 0 else 1), j)
        send(ref, ref, xb_s.at[rel, j], xb_r.at[rel, j], x_to[dr])

    def xb_arrive(rel, j):
        dr = j // 2
        arrive(grp(dpx(rel, 2), j), xb_s.at[rel, j], xb_r.at[rel, j], x_to[1 - dr])

    cell_group(0)
    w_arrive(0, 0)
    cell_group(1)
    cell_group(2)
    w_arrive(0, 1)
    cell_group(3)
    w_arrive(0, 2)
    relay(0, 0)
    y_group(0)
    w_arrive(1, 0)
    relay(0, 1)
    y_group(1)
    w_arrive(1, 1)
    relay(0, 2)
    y_group(2)
    w_arrive(1, 2)
    relay(0, 3)
    y_group(3)
    w_arrive(2, 0)
    relay(1, 0)
    w_arrive(2, 1)
    relay(1, 1)
    w_arrive(2, 2)
    relay(1, 2)
    relay(1, 3)
    for t in (0, 1, 2):
        w_arrive(3, t)
    for rel in (0, 1):
        for j in range(4):
            xa_arrive(1 - j // 2, rel, j)
            xb_arrive(rel, j)

    for i in range(4):
        rows = x_all[2 * i : 2 * i + 2].reshape(256, width)
        first = lax.dot_general(
            rows, w_all[...].reshape(384, width), (((1,), (1,)), ((), ())), preferred_element_type=F32
        ).reshape(16, 2, CAP, 384)
        pre = first[:, 0, :, 0:128]
        upward = first[:, 0, :, 128:256]
        dhidden = first[:, 1, :, 256:384]
        sigmoid = jax.nn.sigmoid(pre)
        swish = pre * sigmoid
        slope = sigmoid * (1.0 + pre * (1.0 - sigmoid))
        active = swish * upward
        dgate = dhidden * upward * slope
        dupward = dhidden * swish
        zero = jnp.zeros_like(active)
        top = jnp.concatenate([dgate, dupward, zero], axis=2)
        low = jnp.concatenate([zero, zero, active], axis=2)
        both = jnp.concatenate([top[:, None], low[:, None]], axis=1).reshape(256, 384)
        lt[:, i * 256 : (i + 1) * 256] = both.T.astype(BF)
        pair[i * 128 : (i + 1) * 128, :] = top.reshape(128, 384)[:, :256].astype(BF)

    tile = 256

    def grad_tile(n, carry):
        cols = pl.ds(pl.multiple_of(n * tile, tile), tile)
        g = jnp.dot(lt[...], x_all[:, :, :, cols].reshape(1024, tile), preferred_element_type=F32)
        grad[:, :, :, cols] = g.reshape(3, 8, 16, tile)
        return carry

    lax.fori_loop(0, width // tile, grad_tile, 0)

    def zg_refs(dr, k, t):
        if k == 0:
            cols = pl.ds(dr * half, half)
            return zs.at[dr, k, t, :, cols], zr.at[dr, k, t, :, cols]
        return zs.at[dr, k, t], zr.at[dr, k, t]

    def zg_send(dr, k, t):
        src, dst = zg_refs(dr, k, t)
        send(src, dst, zg_s.at[dr, k, t], zg_r.at[dr, k, t], z_to[dr])

    def zg_arrive(dr, k, t):
        arrive(zg_refs(dr, k, t)[1], zg_s.at[dr, k, t], zg_r.at[dr, k, t], z_to[1 - dr])

    for t in range(3):
        for dr in (0, 1):
            zs[dr, 0, t, :, dr * half : (dr + 1) * half] = grad[
                t, ring(4), :, dr * half : (dr + 1) * half
            ].astype(BF)
            zg_send(dr, 0, t)

    def zg_step(k, t):
        for dr in (0, 1):
            zg_arrive(dr, k - 1, t)
            c = ring((4 - k) if dr == 0 else (k - 4))
            if k == 1:
                a, b = dr * half, (dr + 1) * half
                oa, ob = (1 - dr) * half, (2 - dr) * half
                zs[dr, k, t, :, a:b] = (grad[t, c, :, a:b] + zr[dr, 0, t, :, a:b].astype(F32)).astype(BF)
                zs[dr, k, t, :, oa:ob] = grad[t, c, :, oa:ob].astype(BF)
            else:
                zs[dr, k, t] = (grad[t, c] + zr[dr, k - 1, t].astype(F32)).astype(BF)
            zg_send(dr, k, t)

    def part_tile(i, carry):
        p = jnp.dot(
            pair[pl.ds(pl.multiple_of(i * 128, 128), 128), :],
            w_all[0:2].reshape(256, width),
            preferred_element_type=F32,
        )
        part[pl.ds(i * 2, 2)] = p.reshape(2, 64, width)
        return carry

    lax.fori_loop(0, 4, part_tile, 0)

    for rel in (1, 0):
        for dr in (0, 1):
            ps0[dr, rel] = part[dpx(rel, 2), dr * 32 : (dr + 1) * 32].astype(BF)
            send(ps0.at[dr, rel], pr0.at[dr, rel], p0_s.at[dr, rel], p0_r.at[dr, rel], x_to[dr])

    def p1_send(dr, rel, h):
        send(ps1.at[dr, rel, h], pr1.at[dr, rel, h], p1_s.at[dr, rel, h], p1_r.at[dr, rel, h], x_to[dr])

    for rel in (1, 0):
        for dr in (0, 1):
            h = 1 - dr
            ps1[dr, rel, h] = part[dpx(rel, 1 if dr == 0 else -1), h * 32 : (h + 1) * 32].astype(BF)
            p1_send(dr, rel, h)

    def p1_step(rel):
        for dr in (0, 1):
            arrive(pr0.at[dr, rel], p0_s.at[dr, rel], p0_r.at[dr, rel], x_to[1 - dr])
            h = dr
            mine = part[dpx(rel, 1 if dr == 0 else -1), h * 32 : (h + 1) * 32]
            ps1[dr, rel, h] = (mine + pr0[dr, rel].astype(F32)).astype(BF)
            p1_send(dr, rel, h)

    def p2_sum(rel, h):
        for dr in (0, 1):
            arrive(
                pr1.at[dr, rel, h], p1_s.at[dr, rel, h], p1_r.at[dr, rel, h], x_to[1 - dr]
            )
        return (
            part[dpx(rel, 0), h * 32 : (h + 1) * 32]
            + pr1[0, rel, h].astype(F32)
            + pr1[1, rel, h].astype(F32)
        )

    for t in range(3):
        zg_step(1, t)
    p1_step(1)
    p1_step(0)
    for t in range(3):
        zg_step(2, t)
    for h in (0, 1):
        ys[h] = p2_sum(1, h).astype(BF)
        send(ys.at[h], yr.at[h], yb_s.at[h], yb_r.at[h], y_to)
    for t in range(3):
        zg_step(3, t)
    for h in (0, 1):
        mine = p2_sum(0, h)
        arrive(yr.at[h], yb_s.at[h], yb_r.at[h], y_to)
        total = mine + yr[h].astype(F32)
        bs[h * 4 : (h + 1) * 4] = total.reshape(4, CAP, width).astype(BF)
    for i in range(1, 8):
        send(bs.at[flip(FLIPS[i])], br.at[e], cb_s.at[i], cb_r.at[i], c_to[i])
    br[e] = bs[e]

    def fg_send_x(rel, t):
        for dr in (0, 1):
            ref = fg.at[t, dpx(rel, 0)]
            send(ref, ref, xg_s.at[dr, rel, t], xg_r.at[dr, rel, t], x_to[dr])

    for t in range(3):
        zg_arrive(0, 3, t)
        zg_arrive(1, 3, t)
        fg[t, dp] = (grad[t, s] + zr[0, 3, t].astype(F32) + zr[1, 3, t].astype(F32)).astype(BF)
        ref = fg.at[t, dp]
        send(ref, ref, yg_s.at[t], yg_r.at[t], y_to)
        fg_send_x(0, t)

    for i in range(1, 8):
        arrive(br.at[flip(FLIPS[i])], cb_s.at[i], cb_r.at[i], c_to[i])
    gi_ref[...] = jnp.dot(
        placed[:, :64].astype(BF),
        br[...].astype(F32).reshape(64, width).astype(BF),
        preferred_element_type=F32,
    ).astype(BF)

    for t in range(3):
        arrive(fg.at[t, dpx(1, 0)], yg_s.at[t], yg_r.at[t], y_to)
        fg_send_x(1, t)

    def far(dr, rel, t, k):
        ref = fg.at[t, dpx(rel, k)]
        if t == 2:
            ref = fg.at[t, dpx(rel, k), :, pl.ds(dr * half, half)]
        return ref

    for rel in (0, 1):
        for t in range(3):
            for dr in (0, 1):
                k = -1 if dr == 0 else 1
                arrive(fg.at[t, dpx(rel, k)], xg_s.at[dr, rel, t], xg_r.at[dr, rel, t], x_to[1 - dr])
                if t == 2 or t == dr:
                    ref = far(dr, rel, t, k)
                    send(ref, ref, xh_s.at[dr, rel, t // 2], xh_r.at[dr, rel, t // 2], x_to[dr])
    for rel in (0, 1):
        for t in range(3):
            for dr in (0, 1):
                if t == 2 or t == dr:
                    arrive(far(dr, rel, t, 2), xh_s.at[dr, rel, t // 2], xh_r.at[dr, rel, t // 2], x_to[1 - dr])
    for c in sends:
        c.wait_send()


def local(tokens, cotangent, expert_ids, gate_probs, gate_weight, up_weight, down_weight):
    rows, width = tokens.shape
    hid = down_weight.shape[1]
    v = pl.BlockSpec(memory_space=pltpu.VMEM)
    a = pl.BlockSpec(memory_space=pl.ANY)
    vm = pltpu.VMEM
    grad_input, grads = pl.pallas_call(
        kernel,
        out_shape=(
            jax.ShapeDtypeStruct((rows, width), BF),
            jax.ShapeDtypeStruct((3, 8, 16, width), BF),
        ),
        in_specs=[v, v, a, a, a, a, a],
        out_specs=(v, v),
        scratch_shapes=[
            vm((rows, width), BF),
            vm((rows, width), BF),
            vm((width, hid), BF),
            vm((width, hid), BF),
            vm((hid, width), BF),
            vm((8, 16, width), BF),
            vm((8, 8, 16, width), BF),
            vm((3, 8, 16, width), BF),
            vm((384, 1024), BF),
            vm((512, 256), BF),
            vm((3, 8, 16, width), F32),
            vm((8, 64, width), F32),
            vm((2, 4, 3, 16, width), BF),
            vm((2, 4, 3, 16, width), BF),
            vm((2, 2, 32, width), BF),
            vm((2, 2, 32, width), BF),
            vm((2, 2, 2, 32, width), BF),
            vm((2, 2, 2, 32, width), BF),
            vm((2, 32, width), BF),
            vm((2, 32, width), BF),
            vm((8, 8, width), BF),
            vm((8, 8, width), BF),
            DMA((5,)),
            DMA((2, 4, 3)),
            DMA((2, 4, 3)),
            DMA((8,)),
            DMA((8,)),
            DMA((4,)),
            DMA((4,)),
            DMA((2, 2, 4)),
            DMA((2, 2, 4)),
            DMA((2, 4)),
            DMA((2, 4)),
            DMA((2, 4, 3)),
            DMA((2, 4, 3)),
            DMA((2, 2)),
            DMA((2, 2)),
            DMA((2, 2, 2)),
            DMA((2, 2, 2)),
            DMA((2,)),
            DMA((2,)),
            DMA((8,)),
            DMA((8,)),
            DMA((3,)),
            DMA((3,)),
            DMA((2, 2, 3)),
            DMA((2, 2, 3)),
            DMA((2, 2, 2)),
            DMA((2, 2, 2)),
        ],
        compiler_params=pltpu.CompilerParams(
            collective_id=0, has_side_effects=True, vmem_limit_bytes=60 * 1024 * 1024
        ),
    )(expert_ids, gate_probs, tokens, cotangent, gate_weight, up_weight, down_weight)
    grads = grads.reshape(3, hid, width)
    return (grad_input, grads[0].T[None], grads[1].T[None], grads[2][None])


def solution(mesh):
    tok = P(("dp", "expert"), None)
    wgt = P("expert", None, None)
    return jax.shard_map(
        local,
        mesh=mesh,
        in_specs=(tok, tok, tok, tok, wgt, wgt, wgt),
        out_specs=(tok, wgt, wgt, wgt),
        check_vma=False,
    )
```

```python
import jax
import jax.numpy as jnp
from jax import lax
from jax.experimental import pallas as pl
from jax.experimental.pallas import tpu as pltpu
from jax.sharding import PartitionSpec as P

SLICES = 8
CAP = 8
XS = 4
BF = jnp.bfloat16
F32 = jnp.float32
MESH = pl.DeviceIdType.MESH
DMA = pltpu.SemaphoreType.DMA
ALL = [(0, 1), (0, -1), (1, 0), (0, 2), (1, 1), (1, -1), (1, 2)]
FLIPS = [(fz, fy, fc) for fz in (0, 1) for fy in (0, 1) for fc in (0, 1)]


def kernel(
    ids_ref,
    probs_ref,
    tok_hbm,
    cot_hbm,
    gate_hbm,
    up_hbm,
    down_hbm,
    gi_ref,
    gg_ref,
    gu_ref,
    gd_ref,
    tok,
    cot,
    gate,
    up,
    msg,
    x_all,
    w_all,
    lt,
    pair,
    grad,
    part,
    zs,
    zr,
    ps0,
    pr0,
    ps1,
    pr1,
    ys,
    yr,
    bs,
    br,
    load_sem,
    za_s,
    za_r,
    ca_s,
    ca_r,
    ya_s,
    ya_r,
    xa_s,
    xa_r,
    xb_s,
    xb_r,
    yx_s,
    yx_r,
    zg_s,
    zg_r,
    p0_s,
    p0_r,
    p1_s,
    p1_r,
    yb_s,
    yb_r,
    cb_s,
    cb_r,
    yg_s,
    yg_r,
    xg_s,
    xg_r,
    xh_s,
    xh_r,
    dg_s,
    dg_r,
):
    fg = (gg_ref, gu_ref, gd_ref)
    width = tok.shape[1]
    half = width // 2
    dp = lax.axis_index("dp")
    ex = lax.axis_index("expert")
    s = ex // 8
    e = ex % 8
    zb, yl, co = e // 4, (e // 2) % 2, e % 2
    x, yh = dp % XS, dp // XS
    oyh = 1 - yh

    def ring(k):
        return (s + k + 8) % 8

    def flip(f):
        fz, fy, fc = f
        return ((zb + fz) % 2) * 4 + ((yl + fy) % 2) * 2 + (co + fc) % 2

    def group(j):
        return ((zb + j // 2) % 2) * 2 + (yl + j % 2) % 2

    def dpx(rel, k):
        return (oyh if rel else yh) * XS + (x + k + XS) % XS

    z_to = [(dp, ring(1) * 8 + e), (dp, ring(-1) * 8 + e)]
    x_to = [(dpx(0, 1), ex), (dpx(0, -1), ex)]
    y_to = (dpx(1, 0), ex)
    all_to = [(dpx(rel, k), ex) for rel, k in ALL]
    far_to = [(dpx(rel, k), ex) for rel, k in ALL[3:]]
    c_to = [(dp, s * 8 + flip(f)) for f in FLIPS]
    sends = []

    def send(src, dst, ssem, rsem, to):
        c = pltpu.make_async_remote_copy(
            src_ref=src, dst_ref=dst, send_sem=ssem, recv_sem=rsem, device_id=to, device_id_type=MESH
        )
        c.start()
        sends.append(c)

    def arrive(dst, ssem, rsem, frm):
        pltpu.make_async_remote_copy(
            src_ref=dst, dst_ref=dst, send_sem=ssem, recv_sem=rsem, device_id=frm, device_id_type=MESH
        ).wait_recv()

    piece = down_hbm.at[0, pl.ds(pl.multiple_of(dp * 16, 16), 16)]
    loads = [
        pltpu.make_async_copy(a, b, load_sem.at[i])
        for i, (a, b) in enumerate(
            [(piece, w_all.at[2, s]), (tok_hbm, tok), (cot_hbm, cot), (gate_hbm.at[0], gate), (up_hbm.at[0], up)]
        )
    ]
    for c in loads:
        c.start()

    barrier = pltpu.get_barrier_semaphore()
    partners = z_to + x_to + [y_to] + c_to[1:] + far_to
    for to in partners:
        pl.semaphore_signal(barrier, inc=1, device_id=to, device_id_type=MESH)

    ids = ids_ref[...]
    probs = probs_ref[...]
    want = lax.broadcasted_iota(jnp.int32, (64, 128), 0) // CAP
    slot = (lax.broadcasted_iota(jnp.int32, (64, 128), 0) % CAP).astype(F32)
    hit = jnp.zeros((64, 128), F32)
    chosen = jnp.zeros((64, 128), F32)
    for k in range(ids.shape[0]):
        m = ids[k : k + 1, :] == want
        hit = hit + jnp.where(m, 1.0, 0.0)
        chosen = chosen + jnp.where(m, probs[k : k + 1, :], 0.0)
    before = jnp.where(
        lax.broadcasted_iota(jnp.int32, (128, 128), 0) < lax.broadcasted_iota(jnp.int32, (128, 128), 1),
        1.0,
        0.0,
    ).astype(BF)
    rank = jnp.dot(hit.astype(BF), before, preferred_element_type=F32)
    placed = jnp.where((hit == 1.0) & (rank == slot), 1.0, 0.0)
    picker = placed.astype(BF)
    prob = jnp.sum(placed * chosen, axis=1, keepdims=True)

    pl.semaphore_wait(barrier, len(partners))

    def w_send(dr, k, t):
        c = ring(-k if dr == 0 else k)
        ref = w_all.at[t, c] if k < 3 else w_all.at[t, c, :, pl.ds(dr * half, half)]
        send(ref, ref, za_s.at[dr, k, t], za_r.at[dr, k, t], z_to[dr])

    def w_arrive(k, t):
        for dr in (0, 1):
            c = ring(-1 - k if dr == 0 else 1 + k)
            ref = w_all.at[t, c] if k < 3 else w_all.at[t, c, :, pl.ds(dr * half, half)]
            arrive(ref, za_s.at[dr, k, t], za_r.at[dr, k, t], z_to[1 - dr])
            if k < 3:
                w_send(dr, k + 1, t)

    loads[0].wait()
    for dr in (0, 1):
        w_send(dr, 0, 2)

    loads[1].wait()
    rows_in = jnp.dot(picker, tok[...], preferred_element_type=F32)
    loads[2].wait()
    rows_cot = prob * jnp.dot(picker, cot[...], preferred_element_type=F32)
    msg[...] = jnp.concatenate(
        [rows_in.reshape(8, CAP, width), rows_cot.reshape(8, CAP, width)], axis=1
    ).astype(BF)
    for i in range(1, 8):
        send(msg.at[flip(FLIPS[i])], x_all.at[dp, e], ca_s.at[i], ca_r.at[i], c_to[i])
    x_all[dp, e] = msg[e]

    def unit(d, u):
        first, n = [(e, 1), (flip((0, 0, 1)), 1), (group(1) * 2, 2), (group(2) * 2, 2),
                    (flip((1, 1, 0)), 1), (flip((1, 1, 1)), 1)][u]
        return x_all.at[d, pl.ds(first, n)]

    def xa_send(rel, u):
        for dr in (0, 1):
            ref = unit(dpx(rel, 0), u)
            send(ref, ref, xa_s.at[dr, rel, u], xa_r.at[dr, rel, u], x_to[dr])

    def own(u):
        for i in [(), (1,), (2, 3), (4, 5), (6,), (7,)][u]:
            arrive(x_all.at[dp, flip(FLIPS[i])], ca_s.at[i], ca_r.at[i], c_to[i])
        xa_send(0, u)
        ref = unit(dp, u)
        send(ref, ref, ya_s.at[u], ya_r.at[u], y_to)

    def yx_send(u, i, k):
        ref = unit(dpx(0, k), u)
        send(ref, ref, yx_s.at[u, i], yx_r.at[u, i], y_to)

    def y_in(u):
        arrive(unit(dpx(1, 0), u), ya_s.at[u], ya_r.at[u], y_to)
        if u >= 2:
            xa_send(1, u)

    def x_in(dr, rel, u):
        k = -1 if dr == 0 else 1
        ref = unit(dpx(rel, k), u)
        arrive(ref, xa_s.at[dr, rel, u], xa_r.at[dr, rel, u], x_to[1 - dr])
        if u % 2 == dr:
            send(ref, ref, xb_s.at[rel, u], xb_r.at[rel, u], x_to[dr])
        if u < 2:
            yx_send(u, dr, k)

    def far_in(rel, u):
        dr = u % 2
        arrive(unit(dpx(rel, 2), u), xb_s.at[rel, u], xb_r.at[rel, u], x_to[1 - dr])
        if u < 2:
            yx_send(u, 2, 2)

    def yx_in(i, k):
        for u in (0, 1):
            arrive(unit(dpx(1, k), u), yx_s.at[u, i], yx_r.at[u, i], y_to)

    own(0)

    row = lax.broadcasted_iota(jnp.int32, (16, 128), 0)
    lane = lax.broadcasted_iota(jnp.int32, (16, 128), 1)
    sel = jnp.where(lane == row + dp * 16, 1.0, 0.0).astype(BF)
    for t, ref in ((0, gate), (1, up)):
        loads[3 + t].wait()
        w_all[t, s] = lax.dot_general(
            sel, ref[...], (((1,), (1,)), ((), ())), preferred_element_type=F32
        ).astype(BF)
        for dr in (0, 1):
            w_send(dr, 0, t)

    own(1)
    own(2)
    own(3)
    x_in(0, 0, 0)
    w_arrive(0, 2)
    x_in(1, 0, 1)
    x_in(1, 0, 0)
    x_in(0, 0, 1)
    own(4)
    own(5)
    w_arrive(0, 0)
    far_in(0, 0)
    far_in(0, 1)
    w_arrive(0, 1)
    y_in(2)
    x_in(0, 0, 2)
    w_arrive(1, 2)
    y_in(3)
    x_in(1, 0, 3)
    w_arrive(1, 0)
    y_in(4)
    y_in(5)
    x_in(0, 0, 4)
    x_in(1, 0, 5)
    w_arrive(1, 1)
    w_arrive(2, 2)
    x_in(0, 1, 2)
    w_arrive(2, 0)
    x_in(1, 1, 3)
    w_arrive(2, 1)
    x_in(0, 1, 4)
    x_in(1, 1, 5)
    for t in (2, 0, 1):
        w_arrive(3, t)

    def compute(k):
        d = (dpx(0, k), dpx(1, k))
        rows = jnp.concatenate([x_all[i].reshape(128, width) for i in d], axis=0)
        first = lax.dot_general(
            rows, w_all[...].reshape(384, width), (((1,), (1,)), ((), ())), preferred_element_type=F32
        ).reshape(16, 2, CAP, 384)
        pre = first[:, 0, :, 0:128]
        upward = first[:, 0, :, 128:256]
        dhidden = first[:, 1, :, 256:384]
        sigmoid = jax.nn.sigmoid(pre)
        swish = pre * sigmoid
        slope = sigmoid * (1.0 + pre * (1.0 - sigmoid))
        active = swish * upward
        dgate = dhidden * upward * slope
        dupward = dhidden * swish
        zero = jnp.zeros_like(active)
        top = jnp.concatenate([dgate, dupward, zero], axis=2)
        low = jnp.concatenate([zero, zero, active], axis=2)
        both = jnp.concatenate([top[:, None], low[:, None]], axis=1).reshape(256, 384).T.astype(BF)
        pairs = top.reshape(128, 384)[:, :256].astype(BF)
        for i in (0, 1):
            lt[:, pl.ds(pl.multiple_of(d[i] * 128, 128), 128)] = both[:, i * 128 : (i + 1) * 128]
            pair[pl.ds(pl.multiple_of(d[i] * 64, 64), 64), :] = pairs[i * 64 : (i + 1) * 64]

    y_in(0)
    y_in(1)
    compute(0)
    for dr in (0, 1):
        for rel in (0, 1):
            for u in (2, 3, 4, 5):
                if u % 2 != dr:
                    x_in(dr, rel, u)
        yx_in(dr, -1 if dr == 0 else 1)
        compute(-1 if dr == 0 else 1)
    for rel in (0, 1):
        for u in (2, 3, 4, 5):
            far_in(rel, u)
    yx_in(2, 2)
    compute(2)

    tile = 256

    def grad_tile(n, carry):
        cols = pl.ds(pl.multiple_of(n * tile, tile), tile)
        g = jnp.dot(lt[...], x_all[:, :, :, cols].reshape(1024, tile), preferred_element_type=F32)
        grad[:, :, :, cols] = g.reshape(3, 8, 16, tile)
        return carry

    def zg_refs(dr, k, t):
        if k == 0:
            cols = pl.ds(dr * half, half)
            return zs.at[dr, k, t, :, cols], zr.at[dr, k, t, :, cols]
        return zs.at[dr, k, t], zr.at[dr, k, t]

    def zg_send(dr, k, t):
        src, dst = zg_refs(dr, k, t)
        send(src, dst, zg_s.at[dr, k, t], zg_r.at[dr, k, t], z_to[dr])

    def zg_arrive(dr, k, t):
        arrive(zg_refs(dr, k, t)[1], zg_s.at[dr, k, t], zg_r.at[dr, k, t], z_to[1 - dr])

    steps = width // tile // 2
    for dr in (0, 1):
        lax.fori_loop(dr * steps, (dr + 1) * steps, grad_tile, 0)
        for t in range(3):
            zs[dr, 0, t, :, dr * half : (dr + 1) * half] = grad[
                t, ring(4), :, dr * half : (dr + 1) * half
            ].astype(BF)
            zg_send(dr, 0, t)

    def zg_step(k, t):
        for dr in (0, 1):
            zg_arrive(dr, k - 1, t)
            c = ring((4 - k) if dr == 0 else (k - 4))
            if k == 1:
                a, b = dr * half, (dr + 1) * half
                oa, ob = (1 - dr) * half, (2 - dr) * half
                zs[dr, k, t, :, a:b] = (grad[t, c, :, a:b] + zr[dr, 0, t, :, a:b].astype(F32)).astype(BF)
                zs[dr, k, t, :, oa:ob] = grad[t, c, :, oa:ob].astype(BF)
            else:
                zs[dr, k, t] = (grad[t, c] + zr[dr, k - 1, t].astype(F32)).astype(BF)
            zg_send(dr, k, t)

    def part_tile(i, carry):
        p = jnp.dot(
            pair[pl.ds(pl.multiple_of(i * 128, 128), 128), :],
            w_all[0:2].reshape(256, width),
            preferred_element_type=F32,
        )
        part[pl.ds(i * 2, 2)] = p.reshape(2, 64, width)
        return carry

    lax.fori_loop(0, 4, part_tile, 0)

    for rel in (1, 0):
        for dr in (0, 1):
            ps0[dr, rel] = part[dpx(rel, 2), dr * 32 : (dr + 1) * 32].astype(BF)
            send(ps0.at[dr, rel], pr0.at[dr, rel], p0_s.at[dr, rel], p0_r.at[dr, rel], x_to[dr])

    def p1_send(dr, rel, h):
        send(ps1.at[dr, rel, h], pr1.at[dr, rel, h], p1_s.at[dr, rel, h], p1_r.at[dr, rel, h], x_to[dr])

    for rel in (1, 0):
        for dr in (0, 1):
            h = 1 - dr
            ps1[dr, rel, h] = part[dpx(rel, 1 if dr == 0 else -1), h * 32 : (h + 1) * 32].astype(BF)
            p1_send(dr, rel, h)

    def p1_step(rel):
        for dr in (0, 1):
            arrive(pr0.at[dr, rel], p0_s.at[dr, rel], p0_r.at[dr, rel], x_to[1 - dr])
            h = dr
            mine = part[dpx(rel, 1 if dr == 0 else -1), h * 32 : (h + 1) * 32]
            ps1[dr, rel, h] = (mine + pr0[dr, rel].astype(F32)).astype(BF)
            p1_send(dr, rel, h)

    def p2_sum(rel, h):
        for dr in (0, 1):
            arrive(
                pr1.at[dr, rel, h], p1_s.at[dr, rel, h], p1_r.at[dr, rel, h], x_to[1 - dr]
            )
        return (
            part[dpx(rel, 0), h * 32 : (h + 1) * 32]
            + pr1[0, rel, h].astype(F32)
            + pr1[1, rel, h].astype(F32)
        )

    for t in range(3):
        zg_step(1, t)
    p1_step(1)
    p1_step(0)
    for t in range(3):
        zg_step(2, t)
    for h in (0, 1):
        ys[h] = p2_sum(1, h).astype(BF)
        send(ys.at[h], yr.at[h], yb_s.at[h], yb_r.at[h], y_to)
    for t in range(3):
        zg_step(3, t)
    for h in (0, 1):
        mine = p2_sum(0, h)
        arrive(yr.at[h], yb_s.at[h], yb_r.at[h], y_to)
        total = mine + yr[h].astype(F32)
        bs[h * 4 : (h + 1) * 4] = total.reshape(4, CAP, width).astype(BF)
    for i in range(1, 8):
        send(bs.at[flip(FLIPS[i])], br.at[e], cb_s.at[i], cb_r.at[i], c_to[i])
    br[e] = bs[e]

    def fg_send_x(rel, t):
        for dr in (0, 1):
            ref = fg[t].at[dpx(rel, 0)]
            send(ref, ref, xg_s.at[dr, rel, t], xg_r.at[dr, rel, t], x_to[dr])

    for t in range(3):
        zg_arrive(0, 3, t)
        zg_arrive(1, 3, t)
        fg[t][dp] = (grad[t, s] + zr[0, 3, t].astype(F32) + zr[1, 3, t].astype(F32)).astype(BF)
        ref = fg[t].at[dp]
        if t < 2:
            send(ref, ref, yg_s.at[t], yg_r.at[t], y_to)
            fg_send_x(0, t)
        else:
            for i, to in enumerate(all_to):
                send(ref, ref, dg_s.at[i], dg_r.at[i], to)

    for i in range(1, 8):
        arrive(br.at[flip(FLIPS[i])], cb_s.at[i], cb_r.at[i], c_to[i])
    gi_ref[...] = lax.dot_general(
        picker,
        br[...].astype(F32).reshape(64, width).astype(BF),
        (((0,), (0,)), ((), ())),
        preferred_element_type=F32,
    ).astype(BF)

    for t in (0, 1):
        arrive(fg[t].at[dpx(1, 0)], yg_s.at[t], yg_r.at[t], y_to)
        fg_send_x(1, t)
    for rel in (0, 1):
        for t in (0, 1):
            for dr in (0, 1):
                k = -1 if dr == 0 else 1
                ref = fg[t].at[dpx(rel, k)]
                arrive(ref, xg_s.at[dr, rel, t], xg_r.at[dr, rel, t], x_to[1 - dr])
                if t == dr:
                    send(ref, ref, xh_s.at[rel, t], xh_r.at[rel, t], x_to[dr])
    for rel in (0, 1):
        for t in (0, 1):
            arrive(fg[t].at[dpx(rel, 2)], xh_s.at[rel, t], xh_r.at[rel, t], x_to[1 - t])
    for i, (rel, k) in enumerate(ALL):
        arrive(fg[2].at[dpx(rel, -k)], dg_s.at[i], dg_r.at[i], (dpx(rel, -k), ex))
    for c in sends:
        c.wait_send()


def local(tokens, cotangent, expert_ids, gate_probs, gate_weight, up_weight, down_weight):
    rows, width = tokens.shape
    hid = down_weight.shape[1]
    v = pl.BlockSpec(memory_space=pltpu.VMEM)
    a = pl.BlockSpec(memory_space=pl.ANY)
    vm = pltpu.VMEM
    grad = jax.ShapeDtypeStruct((8, 16, width), BF)
    grad_input, *grads = pl.pallas_call(
        kernel,
        out_shape=(
            jax.ShapeDtypeStruct((rows, width), BF),
            grad,
            grad,
            grad,
        ),
        in_specs=[v, v, a, a, a, a, a],
        out_specs=(v, v, v, v),
        scratch_shapes=[
            vm((rows, width), BF),
            vm((rows, width), BF),
            vm((width, hid), BF),
            vm((width, hid), BF),
            vm((8, 16, width), BF),
            vm((8, 8, 16, width), BF),
            vm((3, 8, 16, width), BF),
            vm((384, 1024), BF),
            vm((512, 256), BF),
            vm((3, 8, 16, width), F32),
            vm((8, 64, width), F32),
            vm((2, 4, 3, 16, width), BF),
            vm((2, 4, 3, 16, width), BF),
            vm((2, 2, 32, width), BF),
            vm((2, 2, 32, width), BF),
            vm((2, 2, 2, 32, width), BF),
            vm((2, 2, 2, 32, width), BF),
            vm((2, 32, width), BF),
            vm((2, 32, width), BF),
            vm((8, 8, width), BF),
            vm((8, 8, width), BF),
            DMA((5,)),
            DMA((2, 4, 3)),
            DMA((2, 4, 3)),
            DMA((8,)),
            DMA((8,)),
            DMA((6,)),
            DMA((6,)),
            DMA((2, 2, 6)),
            DMA((2, 2, 6)),
            DMA((2, 6)),
            DMA((2, 6)),
            DMA((2, 3)),
            DMA((2, 3)),
            DMA((2, 4, 3)),
            DMA((2, 4, 3)),
            DMA((2, 2)),
            DMA((2, 2)),
            DMA((2, 2, 2)),
            DMA((2, 2, 2)),
            DMA((2,)),
            DMA((2,)),
            DMA((8,)),
            DMA((8,)),
            DMA((3,)),
            DMA((3,)),
            DMA((2, 2, 3)),
            DMA((2, 2, 3)),
            DMA((2, 2)),
            DMA((2, 2)),
            DMA((7,)),
            DMA((7,)),
        ],
        compiler_params=pltpu.CompilerParams(
            collective_id=0, has_side_effects=True, vmem_limit_bytes=60 * 1024 * 1024
        ),
    )(expert_ids.T, gate_probs.T, tokens, cotangent, gate_weight, up_weight, down_weight)
    grads = [g.reshape(hid, width) for g in grads]
    return (grad_input, grads[0].T[None], grads[1].T[None], grads[2][None])


def solution(mesh):
    tok = P(("dp", "expert"), None)
    wgt = P("expert", None, None)
    return jax.shard_map(
        local,
        mesh=mesh,
        in_specs=(tok, tok, tok, tok, wgt, wgt, wgt),
        out_specs=(tok, wgt, wgt, wgt),
        check_vma=False,
    )
```

```python
import jax
import jax.numpy as jnp
from jax import lax
from jax.experimental import pallas as pl
from jax.experimental.pallas import tpu as pltpu
from jax.sharding import PartitionSpec as P

SLICES = 8
CAP = 8
XS = 4
BF = jnp.bfloat16
F32 = jnp.float32
MESH = pl.DeviceIdType.MESH
DMA = pltpu.SemaphoreType.DMA
ALL = [(0, 1), (0, -1), (1, 0), (0, 2), (1, 1), (1, -1), (1, 2)]
FLIPS = [(fz, fy, fc) for fz in (0, 1) for fy in (0, 1) for fc in (0, 1)]


def kernel(
    ids_ref,
    probs_ref,
    tok_hbm,
    cot_hbm,
    gate_hbm,
    up_hbm,
    down_hbm,
    gi_ref,
    gg_ref,
    gu_ref,
    gd_ref,
    tok,
    cot,
    gate,
    up,
    msg,
    x_all,
    w_all,
    lt,
    pair,
    grad,
    part,
    zs,
    zr,
    ps0,
    pr0,
    ps1,
    pr1,
    ys,
    yr,
    bs,
    br,
    load_sem,
    za_s,
    za_r,
    ca_s,
    ca_r,
    ya_s,
    ya_r,
    xa_s,
    xa_r,
    xb_s,
    xb_r,
    yx_s,
    yx_r,
    zg_s,
    zg_r,
    p0_s,
    p0_r,
    p1_s,
    p1_r,
    yb_s,
    yb_r,
    cb_s,
    cb_r,
    yg_s,
    yg_r,
    xg_s,
    xg_r,
    xh_s,
    xh_r,
    dg_s,
    dg_r,
):
    fg = (gg_ref, gu_ref, gd_ref)
    width = tok.shape[1]
    half = width // 2
    dp = lax.axis_index("dp")
    ex = lax.axis_index("expert")
    s = ex // 8
    e = ex % 8
    zb, yl, co = e // 4, (e // 2) % 2, e % 2
    x, yh = dp % XS, dp // XS
    oyh = 1 - yh

    def ring(k):
        return (s + k + 8) % 8

    def flip(f):
        fz, fy, fc = f
        return ((zb + fz) % 2) * 4 + ((yl + fy) % 2) * 2 + (co + fc) % 2

    def group(j):
        return ((zb + j // 2) % 2) * 2 + (yl + j % 2) % 2

    def dpx(rel, k):
        return (oyh if rel else yh) * XS + (x + k + XS) % XS

    z_to = [(dp, ring(1) * 8 + e), (dp, ring(-1) * 8 + e)]
    x_to = [(dpx(0, 1), ex), (dpx(0, -1), ex)]
    y_to = (dpx(1, 0), ex)
    all_to = [(dpx(rel, k), ex) for rel, k in ALL]
    far_to = [(dpx(rel, k), ex) for rel, k in ALL[3:]]
    c_to = [(dp, s * 8 + flip(f)) for f in FLIPS]
    sends = []

    def send(src, dst, ssem, rsem, to):
        c = pltpu.make_async_remote_copy(
            src_ref=src, dst_ref=dst, send_sem=ssem, recv_sem=rsem, device_id=to, device_id_type=MESH
        )
        c.start()
        sends.append(c)

    def arrive(dst, ssem, rsem, frm):
        pltpu.make_async_remote_copy(
            src_ref=dst, dst_ref=dst, send_sem=ssem, recv_sem=rsem, device_id=frm, device_id_type=MESH
        ).wait_recv()

    piece = down_hbm.at[0, pl.ds(pl.multiple_of(dp * 16, 16), 16)]
    loads = [
        pltpu.make_async_copy(a, b, load_sem.at[i])
        for i, (a, b) in enumerate(
            [(piece, w_all.at[2, s]), (tok_hbm, tok), (cot_hbm, cot), (gate_hbm.at[0], gate), (up_hbm.at[0], up)]
        )
    ]
    for c in loads:
        c.start()

    barrier = pltpu.get_barrier_semaphore()
    partners = z_to + x_to + [y_to] + c_to[1:] + far_to
    for to in partners:
        pl.semaphore_signal(barrier, inc=1, device_id=to, device_id_type=MESH)

    ids = ids_ref[...]
    probs = probs_ref[...]
    want = lax.broadcasted_iota(jnp.int32, (64, 128), 0) // CAP
    slot = (lax.broadcasted_iota(jnp.int32, (64, 128), 0) % CAP).astype(F32)
    hit = jnp.zeros((64, 128), F32)
    chosen = jnp.zeros((64, 128), F32)
    for k in range(ids.shape[0]):
        m = ids[k : k + 1, :] == want
        hit = hit + jnp.where(m, 1.0, 0.0)
        chosen = chosen + jnp.where(m, probs[k : k + 1, :], 0.0)
    before = jnp.where(
        lax.broadcasted_iota(jnp.int32, (128, 128), 0) < lax.broadcasted_iota(jnp.int32, (128, 128), 1),
        1.0,
        0.0,
    ).astype(BF)
    rank = jnp.dot(hit.astype(BF), before, preferred_element_type=F32)
    placed = jnp.where((hit == 1.0) & (rank == slot), 1.0, 0.0)
    picker = placed.astype(BF)
    prob = jnp.sum(placed * chosen, axis=1, keepdims=True)

    pl.semaphore_wait(barrier, len(partners))

    def w_send(dr, k, t):
        c = ring(-k if dr == 0 else k)
        ref = w_all.at[t, c] if k < 3 else w_all.at[t, c, :, pl.ds(dr * half, half)]
        send(ref, ref, za_s.at[dr, k, t], za_r.at[dr, k, t], z_to[dr])

    def w_arrive(k, t):
        for dr in (0, 1):
            c = ring(-1 - k if dr == 0 else 1 + k)
            ref = w_all.at[t, c] if k < 3 else w_all.at[t, c, :, pl.ds(dr * half, half)]
            arrive(ref, za_s.at[dr, k, t], za_r.at[dr, k, t], z_to[1 - dr])
            if k < 3:
                w_send(dr, k + 1, t)

    loads[0].wait()
    for dr in (0, 1):
        w_send(dr, 0, 2)

    loads[1].wait()
    rows_in = jnp.dot(picker, tok[...], preferred_element_type=F32)
    loads[2].wait()
    rows_cot = prob * jnp.dot(picker, cot[...], preferred_element_type=F32)
    msg[...] = jnp.concatenate(
        [rows_in.reshape(8, CAP, width), rows_cot.reshape(8, CAP, width)], axis=1
    ).astype(BF)
    for i in range(1, 8):
        send(msg.at[flip(FLIPS[i])], x_all.at[dp, e], ca_s.at[i], ca_r.at[i], c_to[i])
    x_all[dp, e] = msg[e]

    def unit(d, u):
        first, n = [(e, 1), (flip((0, 0, 1)), 1), (group(1) * 2, 2), (group(2) * 2, 2),
                    (flip((1, 1, 0)), 1), (flip((1, 1, 1)), 1)][u]
        return x_all.at[d, pl.ds(first, n)]

    def xa_send(rel, u):
        for dr in (0, 1):
            ref = unit(dpx(rel, 0), u)
            send(ref, ref, xa_s.at[dr, rel, u], xa_r.at[dr, rel, u], x_to[dr])

    def own(u):
        for i in [(), (1,), (2, 3), (4, 5), (6,), (7,)][u]:
            arrive(x_all.at[dp, flip(FLIPS[i])], ca_s.at[i], ca_r.at[i], c_to[i])
        xa_send(0, u)
        ref = unit(dp, u)
        send(ref, ref, ya_s.at[u], ya_r.at[u], y_to)

    def yx_send(u, i, k):
        ref = unit(dpx(0, k), u)
        send(ref, ref, yx_s.at[u, i], yx_r.at[u, i], y_to)

    def y_in(u):
        arrive(unit(dpx(1, 0), u), ya_s.at[u], ya_r.at[u], y_to)
        if u >= 2:
            xa_send(1, u)

    def x_in(dr, rel, u):
        k = -1 if dr == 0 else 1
        ref = unit(dpx(rel, k), u)
        arrive(ref, xa_s.at[dr, rel, u], xa_r.at[dr, rel, u], x_to[1 - dr])
        if u % 2 == dr:
            send(ref, ref, xb_s.at[rel, u], xb_r.at[rel, u], x_to[dr])
        if u < 2:
            yx_send(u, dr, k)

    def far_in(rel, u):
        dr = u % 2
        arrive(unit(dpx(rel, 2), u), xb_s.at[rel, u], xb_r.at[rel, u], x_to[1 - dr])
        if u < 2:
            yx_send(u, 2, 2)

    def yx_in(i, k):
        for u in (0, 1):
            arrive(unit(dpx(1, k), u), yx_s.at[u, i], yx_r.at[u, i], y_to)

    own(0)

    row = lax.broadcasted_iota(jnp.int32, (16, 128), 0)
    lane = lax.broadcasted_iota(jnp.int32, (16, 128), 1)
    sel = jnp.where(lane == row + dp * 16, 1.0, 0.0).astype(BF)
    for t, ref in ((0, gate), (1, up)):
        loads[3 + t].wait()
        w_all[t, s] = lax.dot_general(
            sel, ref[...], (((1,), (1,)), ((), ())), preferred_element_type=F32
        ).astype(BF)
        for dr in (0, 1):
            w_send(dr, 0, t)

    own(1)
    own(2)
    own(3)
    x_in(0, 0, 0)
    w_arrive(0, 2)
    x_in(1, 0, 1)
    x_in(1, 0, 0)
    x_in(0, 0, 1)
    own(4)
    own(5)
    w_arrive(0, 0)
    far_in(0, 0)
    far_in(0, 1)
    w_arrive(0, 1)
    y_in(2)
    x_in(0, 0, 2)
    w_arrive(1, 2)
    y_in(3)
    x_in(1, 0, 3)
    w_arrive(1, 0)
    y_in(4)
    y_in(5)
    x_in(0, 0, 4)
    x_in(1, 0, 5)
    w_arrive(1, 1)
    w_arrive(2, 2)
    x_in(0, 1, 2)
    w_arrive(2, 0)
    x_in(1, 1, 3)
    w_arrive(2, 1)
    x_in(0, 1, 4)
    x_in(1, 1, 5)
    for t in (2, 0, 1):
        w_arrive(3, t)

    def compute(k):
        d = (dpx(0, k), dpx(1, k))
        rows = jnp.concatenate([x_all[i].reshape(128, width) for i in d], axis=0)
        first = lax.dot_general(
            rows, w_all[...].reshape(384, width), (((1,), (1,)), ((), ())), preferred_element_type=F32
        ).reshape(16, 2, CAP, 384)
        pre = first[:, 0, :, 0:128]
        upward = first[:, 0, :, 128:256]
        dhidden = first[:, 1, :, 256:384]
        sigmoid = jax.nn.sigmoid(pre)
        swish = pre * sigmoid
        slope = sigmoid * (1.0 + pre * (1.0 - sigmoid))
        active = swish * upward
        dgate = dhidden * upward * slope
        dupward = dhidden * swish
        zero = jnp.zeros_like(active)
        top = jnp.concatenate([dgate, dupward, zero], axis=2)
        low = jnp.concatenate([zero, zero, active], axis=2)
        both = jnp.concatenate([top[:, None], low[:, None]], axis=1).reshape(256, 384).T.astype(BF)
        pairs = top.reshape(128, 384)[:, :256].astype(BF)
        for i in (0, 1):
            lt[:, pl.ds(pl.multiple_of(d[i] * 128, 128), 128)] = both[:, i * 128 : (i + 1) * 128]
            pair[pl.ds(pl.multiple_of(d[i] * 64, 64), 64), :] = pairs[i * 64 : (i + 1) * 64]

    y_in(0)
    y_in(1)
    compute(0)
    for dr in (0, 1):
        for rel in (0, 1):
            for u in (2, 3, 4, 5):
                if u % 2 != dr:
                    x_in(dr, rel, u)
        yx_in(dr, -1 if dr == 0 else 1)
        compute(-1 if dr == 0 else 1)
    for rel in (0, 1):
        for u in (2, 3, 4, 5):
            far_in(rel, u)
    yx_in(2, 2)
    compute(2)

    tile = 256

    def grad_tile(n, carry):
        cols = pl.ds(pl.multiple_of(n * tile, tile), tile)
        g = jnp.dot(lt[...], x_all[:, :, :, cols].reshape(1024, tile), preferred_element_type=F32)
        grad[:, :, :, cols] = g.reshape(3, 8, 16, tile)
        return carry

    def zg_refs(dr, k, t, c):
        cols = pl.ds(c * half, half)
        return zs.at[dr, k, t, :, cols], zr.at[dr, k, t, :, cols]

    def zg_arrive(dr, k, t, c):
        arrive(zg_refs(dr, k, t, c)[1], zg_s.at[dr, k, t, c], zg_r.at[dr, k, t, c], z_to[1 - dr])

    def zg(dr, k, t, c, add):
        a, b = c * half, (c + 1) * half
        value = grad[t, ring((4 - k) if dr == 0 else (k - 4)), :, a:b]
        if add:
            zg_arrive(dr, k - 1, t, c)
            value = value + zr[dr, k - 1, t, :, a:b].astype(F32)
        zs[dr, k, t, :, a:b] = value.astype(BF)
        src, dst = zg_refs(dr, k, t, c)
        send(src, dst, zg_s.at[dr, k, t, c], zg_r.at[dr, k, t, c], z_to[dr])

    steps = width // tile // 2
    for c in (0, 1):
        lax.fori_loop(c * steps, (c + 1) * steps, grad_tile, 0)
        for t in range(3):
            zg(c, 0, t, c, False)
        for t in range(3):
            zg(1 - c, 1, t, c, False)

    def part_tile(i, carry):
        p = jnp.dot(
            pair[pl.ds(pl.multiple_of(i * 128, 128), 128), :],
            w_all[0:2].reshape(256, width),
            preferred_element_type=F32,
        )
        part[pl.ds(i * 2, 2)] = p.reshape(2, 64, width)
        return carry

    lax.fori_loop(0, 4, part_tile, 0)

    for rel in (1, 0):
        for dr in (0, 1):
            ps0[dr, rel] = part[dpx(rel, 2), dr * 32 : (dr + 1) * 32].astype(BF)
            send(ps0.at[dr, rel], pr0.at[dr, rel], p0_s.at[dr, rel], p0_r.at[dr, rel], x_to[dr])

    def p1_send(dr, rel, h):
        send(ps1.at[dr, rel, h], pr1.at[dr, rel, h], p1_s.at[dr, rel, h], p1_r.at[dr, rel, h], x_to[dr])

    for rel in (1, 0):
        for dr in (0, 1):
            h = 1 - dr
            ps1[dr, rel, h] = part[dpx(rel, 1 if dr == 0 else -1), h * 32 : (h + 1) * 32].astype(BF)
            p1_send(dr, rel, h)

    def p1_step(rel):
        for dr in (0, 1):
            arrive(pr0.at[dr, rel], p0_s.at[dr, rel], p0_r.at[dr, rel], x_to[1 - dr])
            h = dr
            mine = part[dpx(rel, 1 if dr == 0 else -1), h * 32 : (h + 1) * 32]
            ps1[dr, rel, h] = (mine + pr0[dr, rel].astype(F32)).astype(BF)
            p1_send(dr, rel, h)

    def p2_sum(rel, h):
        for dr in (0, 1):
            arrive(
                pr1.at[dr, rel, h], p1_s.at[dr, rel, h], p1_r.at[dr, rel, h], x_to[1 - dr]
            )
        return (
            part[dpx(rel, 0), h * 32 : (h + 1) * 32]
            + pr1[0, rel, h].astype(F32)
            + pr1[1, rel, h].astype(F32)
        )

    for t in range(3):
        for dr in (0, 1):
            zg(dr, 1, t, dr, True)
    p1_step(1)

    def zg_all(k, c):
        for t in range(3):
            for dr in (0, 1):
                zg(dr, k, t, c, True)

    zg_all(2, 1)
    p1_step(0)
    zg_all(2, 0)
    for h in (0, 1):
        ys[h] = p2_sum(1, h).astype(BF)
        send(ys.at[h], yr.at[h], yb_s.at[h], yb_r.at[h], y_to)
    zg_all(3, 1)
    for h in (0, 1):
        mine = p2_sum(0, h)
        arrive(yr.at[h], yb_s.at[h], yb_r.at[h], y_to)
        total = mine + yr[h].astype(F32)
        bs[h * 4 : (h + 1) * 4] = total.reshape(4, CAP, width).astype(BF)
    for i in range(1, 8):
        send(bs.at[flip(FLIPS[i])], br.at[e], cb_s.at[i], cb_r.at[i], c_to[i])
    br[e] = bs[e]
    zg_all(3, 0)

    def final(t, c):
        a, b = c * half, (c + 1) * half
        for dr in (0, 1):
            zg_arrive(dr, 3, t, c)
        total = grad[t, s, :, a:b]
        for dr in (0, 1):
            total = total + zr[dr, 3, t, :, a:b].astype(F32)
        fg[t][dp, :, a:b] = total.astype(BF)

    def late(t, rel, k):
        return fg[t].at[dpx(rel, k), :, pl.ds(half, half)]

    def fg_send_x(rel, t):
        for dr in (0, 1):
            ref = late(t, rel, 0)
            send(ref, ref, xg_s.at[dr, rel, t], xg_r.at[dr, rel, t], x_to[dr])

    for t in range(3):
        final(t, 1)
        ref = late(t, 0, 0)
        send(ref, ref, yg_s.at[t], yg_r.at[t], y_to)
        fg_send_x(0, t)

    for i in range(1, 8):
        arrive(br.at[flip(FLIPS[i])], cb_s.at[i], cb_r.at[i], c_to[i])
    gi_ref[...] = lax.dot_general(
        picker,
        br[...].astype(F32).reshape(64, width).astype(BF),
        (((0,), (0,)), ((), ())),
        preferred_element_type=F32,
    ).astype(BF)

    for t in range(3):
        arrive(late(t, 1, 0), yg_s.at[t], yg_r.at[t], y_to)
        fg_send_x(1, t)
    for t in range(3):
        final(t, 0)
        ref = fg[t].at[dp, :, pl.ds(0, half)]
        for i, to in enumerate(all_to):
            send(ref, ref, dg_s.at[t, i], dg_r.at[t, i], to)

    def relayed(t, rel, k, dr):
        if t < 2:
            return late(t, rel, k), t
        return fg[t].at[dpx(rel, k), :, pl.ds(half + dr * (half // 2), half // 2)], 2 + dr

    for rel in (0, 1):
        for t in range(3):
            for dr in (0, 1):
                k = -1 if dr == 0 else 1
                arrive(late(t, rel, k), xg_s.at[dr, rel, t], xg_r.at[dr, rel, t], x_to[1 - dr])
                if t == 2 or t == dr:
                    ref, i = relayed(t, rel, k, dr)
                    send(ref, ref, xh_s.at[rel, i], xh_r.at[rel, i], x_to[dr])
    for rel in (0, 1):
        for t in range(3):
            for dr in (0, 1):
                if t == 2 or t == dr:
                    ref, i = relayed(t, rel, 2, dr)
                    arrive(ref, xh_s.at[rel, i], xh_r.at[rel, i], x_to[1 - dr])
    for t in range(3):
        for i, (rel, k) in enumerate(ALL):
            arrive(
                fg[t].at[dpx(rel, -k), :, pl.ds(0, half)], dg_s.at[t, i], dg_r.at[t, i], (dpx(rel, -k), ex)
            )
    for c in sends:
        c.wait_send()


def finish(gi, gg, gu, gd, gi_out, gg_out, gu_out, gd_out, inner, turned, in_sem, out_sem):
    refs = [(gg, gg_out), (gu, gu_out), (gi, gi_out), (gd, gd_out)]
    ins = [pltpu.make_async_copy(a, inner.at[i], in_sem.at[i]) for i, (a, _) in enumerate(refs)]
    for c in ins:
        c.start()
    outs = []
    for i, (_, b) in enumerate(refs):
        ins[i].wait()
        src = inner.at[i]
        if i < 2:
            turned[i] = inner[i].T
            src = turned.at[i]
        c = pltpu.make_async_copy(src, b, out_sem.at[i])
        c.start()
        outs.append(c)
    for c in outs:
        c.wait()


def local(tokens, cotangent, expert_ids, gate_probs, gate_weight, up_weight, down_weight):
    rows, width = tokens.shape
    hid = down_weight.shape[1]
    v = pl.BlockSpec(memory_space=pltpu.VMEM)
    a = pl.BlockSpec(memory_space=pl.ANY)
    vm = pltpu.VMEM
    grad = jax.ShapeDtypeStruct((8, 16, width), BF)
    grad_input, *grads = pl.pallas_call(
        kernel,
        out_shape=(
            jax.ShapeDtypeStruct((rows, width), BF),
            grad,
            grad,
            grad,
        ),
        in_specs=[v, v, a, a, a, a, a],
        out_specs=(v, v, v, v),
        scratch_shapes=[
            vm((rows, width), BF),
            vm((rows, width), BF),
            vm((width, hid), BF),
            vm((width, hid), BF),
            vm((8, 16, width), BF),
            vm((8, 8, 16, width), BF),
            vm((3, 8, 16, width), BF),
            vm((384, 1024), BF),
            vm((512, 256), BF),
            vm((3, 8, 16, width), F32),
            vm((8, 64, width), F32),
            vm((2, 4, 3, 16, width), BF),
            vm((2, 4, 3, 16, width), BF),
            vm((2, 2, 32, width), BF),
            vm((2, 2, 32, width), BF),
            vm((2, 2, 2, 32, width), BF),
            vm((2, 2, 2, 32, width), BF),
            vm((2, 32, width), BF),
            vm((2, 32, width), BF),
            vm((8, 8, width), BF),
            vm((8, 8, width), BF),
            DMA((5,)),
            DMA((2, 4, 3)),
            DMA((2, 4, 3)),
            DMA((8,)),
            DMA((8,)),
            DMA((6,)),
            DMA((6,)),
            DMA((2, 2, 6)),
            DMA((2, 2, 6)),
            DMA((2, 6)),
            DMA((2, 6)),
            DMA((2, 3)),
            DMA((2, 3)),
            DMA((2, 4, 3, 2)),
            DMA((2, 4, 3, 2)),
            DMA((2, 2)),
            DMA((2, 2)),
            DMA((2, 2, 2)),
            DMA((2, 2, 2)),
            DMA((2,)),
            DMA((2,)),
            DMA((8,)),
            DMA((8,)),
            DMA((3,)),
            DMA((3,)),
            DMA((2, 2, 3)),
            DMA((2, 2, 3)),
            DMA((2, 4)),
            DMA((2, 4)),
            DMA((3, 7)),
            DMA((3, 7)),
        ],
        compiler_params=pltpu.CompilerParams(
            collective_id=0, has_side_effects=True, vmem_limit_bytes=60 * 1024 * 1024
        ),
    )(expert_ids.T, gate_probs.T, tokens, cotangent, gate_weight, up_weight, down_weight)
    flat = jax.ShapeDtypeStruct((hid, width), BF)
    tall = jax.ShapeDtypeStruct((width, hid), BF)
    grads = [g.reshape(hid, width) for g in grads]
    grad_input, gate, up, down = pl.pallas_call(
        finish,
        out_shape=(flat, tall, tall, flat),
        in_specs=[a] * 4,
        out_specs=(a, a, a, a),
        scratch_shapes=[
            vm((4, hid, width), BF),
            vm((2, width, hid), BF),
            DMA((4,)),
            DMA((4,)),
        ],
        compiler_params=pltpu.CompilerParams(vmem_limit_bytes=60 * 1024 * 1024),
    )(grad_input, *grads)
    return (grad_input, gate[None], up[None], down[None])


def solution(mesh):
    tok = P(("dp", "expert"), None)
    wgt = P("expert", None, None)
    return jax.shard_map(
        local,
        mesh=mesh,
        in_specs=(tok, tok, tok, tok, wgt, wgt, wgt),
        out_specs=(tok, wgt, wgt, wgt),
        check_vma=False,
    )
```

```python
import jax
import jax.numpy as jnp
from jax import lax
from jax.experimental import pallas as pl
from jax.experimental.pallas import tpu as pltpu
from jax.sharding import PartitionSpec as P

SLICES = 8
CAP = 8
XS = 4
BF = jnp.bfloat16
F32 = jnp.float32
MESH = pl.DeviceIdType.MESH
DMA = pltpu.SemaphoreType.DMA
ALL = [(0, 1), (0, -1), (1, 0), (0, 2), (1, 1), (1, -1), (1, 2)]
FLIPS = [(fz, fy, fc) for fz in (0, 1) for fy in (0, 1) for fc in (0, 1)]


def kernel(
    ids_hbm,
    probs_hbm,
    tok_hbm,
    cot_hbm,
    gate_hbm,
    up_hbm,
    down_hbm,
    gi_ref,
    gg_ref,
    gu_ref,
    gd_ref,
    ids_ref,
    probs_ref,
    tok,
    cot,
    gate,
    up,
    msg,
    x_all,
    w_all,
    lt,
    pair,
    grad,
    part,
    zs,
    zr,
    ps0,
    pr0,
    ps1,
    pr1,
    ys,
    yr,
    bs,
    br,
    load_sem,
    za_s,
    za_r,
    ca_s,
    ca_r,
    ya_s,
    ya_r,
    xa_s,
    xa_r,
    xb_s,
    xb_r,
    yx_s,
    yx_r,
    zg_s,
    zg_r,
    p0_s,
    p0_r,
    p1_s,
    p1_r,
    yb_s,
    yb_r,
    cb_s,
    cb_r,
    yg_s,
    yg_r,
    xg_s,
    xg_r,
    xh_s,
    xh_r,
    dg_s,
    dg_r,
):
    fg = (gg_ref, gu_ref, gd_ref)
    width = tok.shape[1]
    half = width // 2
    dp = lax.axis_index("dp")
    ex = lax.axis_index("expert")
    s = ex // 8
    e = ex % 8
    zb, yl, co = e // 4, (e // 2) % 2, e % 2
    x, yh = dp % XS, dp // XS
    oyh = 1 - yh

    def ring(k):
        return (s + k + 8) % 8

    def flip(f):
        fz, fy, fc = f
        return ((zb + fz) % 2) * 4 + ((yl + fy) % 2) * 2 + (co + fc) % 2

    def group(j):
        return ((zb + j // 2) % 2) * 2 + (yl + j % 2) % 2

    def dpx(rel, k):
        return (oyh if rel else yh) * XS + (x + k + XS) % XS

    z_to = [(dp, ring(1) * 8 + e), (dp, ring(-1) * 8 + e)]
    x_to = [(dpx(0, 1), ex), (dpx(0, -1), ex)]
    y_to = (dpx(1, 0), ex)
    all_to = [(dpx(rel, k), ex) for rel, k in ALL]
    far_to = [(dpx(rel, k), ex) for rel, k in ALL[3:]]
    c_to = [(dp, s * 8 + flip(f)) for f in FLIPS]
    sends = []

    def send(src, dst, ssem, rsem, to):
        c = pltpu.make_async_remote_copy(
            src_ref=src, dst_ref=dst, send_sem=ssem, recv_sem=rsem, device_id=to, device_id_type=MESH
        )
        c.start()
        sends.append(c)

    def arrive(dst, ssem, rsem, frm):
        pltpu.make_async_remote_copy(
            src_ref=dst, dst_ref=dst, send_sem=ssem, recv_sem=rsem, device_id=frm, device_id_type=MESH
        ).wait_recv()

    barrier = pltpu.get_barrier_semaphore()
    partners = z_to + x_to + [y_to] + c_to[1:] + far_to
    for to in partners:
        pl.semaphore_signal(barrier, inc=1, device_id=to, device_id_type=MESH)

    piece = down_hbm.at[0, pl.ds(pl.multiple_of(dp * 16, 16), 16)]
    loads = [
        pltpu.make_async_copy(a, b, load_sem.at[i])
        for i, (a, b) in enumerate(
            [(piece, w_all.at[2, s]), (tok_hbm, tok), (cot_hbm, cot), (gate_hbm.at[0], gate),
             (up_hbm.at[0], up), (ids_hbm, ids_ref), (probs_hbm, probs_ref)]
        )
    ]
    for i in (5, 6, 0, 1, 2, 3, 4):
        loads[i].start()

    loads[5].wait()
    loads[6].wait()
    ids = ids_ref[...]
    probs = probs_ref[...]
    want = lax.broadcasted_iota(jnp.int32, (64, 128), 0) // CAP
    slot = (lax.broadcasted_iota(jnp.int32, (64, 128), 0) % CAP).astype(F32)
    hit = jnp.zeros((64, 128), F32)
    chosen = jnp.zeros((64, 128), F32)
    for k in range(ids.shape[0]):
        m = ids[k : k + 1, :] == want
        hit = hit + jnp.where(m, 1.0, 0.0)
        chosen = chosen + jnp.where(m, probs[k : k + 1, :], 0.0)
    before = jnp.where(
        lax.broadcasted_iota(jnp.int32, (128, 128), 0) < lax.broadcasted_iota(jnp.int32, (128, 128), 1),
        1.0,
        0.0,
    ).astype(BF)
    rank = jnp.dot(hit.astype(BF), before, preferred_element_type=F32)
    placed = jnp.where((hit == 1.0) & (rank == slot), 1.0, 0.0)
    picker = placed.astype(BF)
    prob = jnp.sum(placed * chosen, axis=1, keepdims=True)

    pl.semaphore_wait(barrier, len(partners))

    def w_send(dr, k, t):
        c = ring(-k if dr == 0 else k)
        ref = w_all.at[t, c] if k < 3 else w_all.at[t, c, :, pl.ds(dr * half, half)]
        send(ref, ref, za_s.at[dr, k, t], za_r.at[dr, k, t], z_to[dr])

    def w_arrive(k, t):
        for dr in (0, 1):
            c = ring(-1 - k if dr == 0 else 1 + k)
            ref = w_all.at[t, c] if k < 3 else w_all.at[t, c, :, pl.ds(dr * half, half)]
            arrive(ref, za_s.at[dr, k, t], za_r.at[dr, k, t], z_to[1 - dr])
            if k < 3:
                w_send(dr, k + 1, t)

    loads[0].wait()
    for dr in (0, 1):
        w_send(dr, 0, 2)

    loads[1].wait()
    rows_in = jnp.dot(picker, tok[...], preferred_element_type=F32)
    loads[2].wait()
    rows_cot = prob * jnp.dot(picker, cot[...], preferred_element_type=F32)
    msg[...] = jnp.concatenate(
        [rows_in.reshape(8, CAP, width), rows_cot.reshape(8, CAP, width)], axis=1
    ).astype(BF)
    for i in range(1, 8):
        send(msg.at[flip(FLIPS[i])], x_all.at[dp, e], ca_s.at[i], ca_r.at[i], c_to[i])
    x_all[dp, e] = msg[e]

    def unit(d, u):
        first, n = [(e, 1), (flip((0, 0, 1)), 1), (group(1) * 2, 2), (group(2) * 2, 2),
                    (flip((1, 1, 0)), 1), (flip((1, 1, 1)), 1)][u]
        return x_all.at[d, pl.ds(first, n)]

    def xa_send(rel, u):
        for dr in (0, 1):
            ref = unit(dpx(rel, 0), u)
            send(ref, ref, xa_s.at[dr, rel, u], xa_r.at[dr, rel, u], x_to[dr])

    def own(u):
        for i in [(), (1,), (2, 3), (4, 5), (6,), (7,)][u]:
            arrive(x_all.at[dp, flip(FLIPS[i])], ca_s.at[i], ca_r.at[i], c_to[i])
        xa_send(0, u)
        ref = unit(dp, u)
        send(ref, ref, ya_s.at[u], ya_r.at[u], y_to)

    def yx_send(u, i, k):
        ref = unit(dpx(0, k), u)
        send(ref, ref, yx_s.at[u, i], yx_r.at[u, i], y_to)

    def y_in(u):
        arrive(unit(dpx(1, 0), u), ya_s.at[u], ya_r.at[u], y_to)
        if u >= 2:
            xa_send(1, u)

    def x_in(dr, rel, u):
        k = -1 if dr == 0 else 1
        ref = unit(dpx(rel, k), u)
        arrive(ref, xa_s.at[dr, rel, u], xa_r.at[dr, rel, u], x_to[1 - dr])
        if u % 2 == dr:
            send(ref, ref, xb_s.at[rel, u], xb_r.at[rel, u], x_to[dr])
        if u < 2:
            yx_send(u, dr, k)

    def far_in(rel, u):
        dr = u % 2
        arrive(unit(dpx(rel, 2), u), xb_s.at[rel, u], xb_r.at[rel, u], x_to[1 - dr])
        if u < 2:
            yx_send(u, 2, 2)

    def yx_in(i, k):
        for u in (0, 1):
            arrive(unit(dpx(1, k), u), yx_s.at[u, i], yx_r.at[u, i], y_to)

    own(0)

    row = lax.broadcasted_iota(jnp.int32, (16, 128), 0)
    lane = lax.broadcasted_iota(jnp.int32, (16, 128), 1)
    sel = jnp.where(lane == row + dp * 16, 1.0, 0.0).astype(BF)
    for t, ref in ((0, gate), (1, up)):
        loads[3 + t].wait()
        w_all[t, s] = lax.dot_general(
            sel, ref[...], (((1,), (1,)), ((), ())), preferred_element_type=F32
        ).astype(BF)
        for dr in (0, 1):
            w_send(dr, 0, t)
        if t == 0:
            own(1)

    own(2)
    own(3)
    x_in(0, 0, 0)
    w_arrive(0, 2)
    x_in(1, 0, 1)
    x_in(1, 0, 0)
    x_in(0, 0, 1)
    own(4)
    own(5)
    w_arrive(0, 0)
    far_in(0, 0)
    far_in(0, 1)
    w_arrive(0, 1)
    y_in(2)
    x_in(0, 0, 2)
    w_arrive(1, 2)
    y_in(3)
    x_in(1, 0, 3)
    w_arrive(1, 0)
    y_in(4)
    y_in(5)
    x_in(0, 0, 4)
    x_in(1, 0, 5)
    w_arrive(1, 1)
    w_arrive(2, 2)
    x_in(0, 1, 2)
    w_arrive(2, 0)
    x_in(1, 1, 3)
    w_arrive(2, 1)
    x_in(0, 1, 4)
    x_in(1, 1, 5)
    for t in (2, 0, 1):
        w_arrive(3, t)

    def compute(k):
        d = (dpx(0, k), dpx(1, k))
        rows = jnp.concatenate([x_all[i].reshape(128, width) for i in d], axis=0)
        first = lax.dot_general(
            rows, w_all[...].reshape(384, width), (((1,), (1,)), ((), ())), preferred_element_type=F32
        ).reshape(16, 2, CAP, 384)
        pre = first[:, 0, :, 0:128]
        upward = first[:, 0, :, 128:256]
        dhidden = first[:, 1, :, 256:384]
        sigmoid = jax.nn.sigmoid(pre)
        swish = pre * sigmoid
        slope = sigmoid * (1.0 + pre * (1.0 - sigmoid))
        active = swish * upward
        dgate = dhidden * upward * slope
        dupward = dhidden * swish
        zero = jnp.zeros_like(active)
        top = jnp.concatenate([dgate, dupward, zero], axis=2)
        low = jnp.concatenate([zero, zero, active], axis=2)
        both = jnp.concatenate([top[:, None], low[:, None]], axis=1).reshape(256, 384).T.astype(BF)
        pairs = top.reshape(128, 384)[:, :256].astype(BF)
        for i in (0, 1):
            lt[:, pl.ds(pl.multiple_of(d[i] * 128, 128), 128)] = both[:, i * 128 : (i + 1) * 128]
            pair[pl.ds(pl.multiple_of(d[i] * 64, 64), 64), :] = pairs[i * 64 : (i + 1) * 64]

    y_in(0)
    y_in(1)
    compute(0)
    for dr in (0, 1):
        for rel in (0, 1):
            for u in (2, 3, 4, 5):
                if u % 2 != dr:
                    x_in(dr, rel, u)
        yx_in(dr, -1 if dr == 0 else 1)
        compute(-1 if dr == 0 else 1)
    for rel in (0, 1):
        for u in (2, 3, 4, 5):
            far_in(rel, u)
    yx_in(2, 2)
    compute(2)

    tile = 256

    def grad_tile(n, carry):
        cols = pl.ds(pl.multiple_of(n * tile, tile), tile)
        g = jnp.dot(lt[...], x_all[:, :, :, cols].reshape(1024, tile), preferred_element_type=F32)
        grad[:, :, :, cols] = g.reshape(3, 8, 16, tile)
        return carry

    def zg_refs(dr, k, t, c):
        cols = pl.ds(c * half, half)
        return zs.at[dr, k, t, :, cols], zr.at[dr, k, t, :, cols]

    def zg_arrive(dr, k, t, c):
        arrive(zg_refs(dr, k, t, c)[1], zg_s.at[dr, k, t, c], zg_r.at[dr, k, t, c], z_to[1 - dr])

    def zg(dr, k, t, c, add):
        a, b = c * half, (c + 1) * half
        value = grad[t, ring((4 - k) if dr == 0 else (k - 4)), :, a:b]
        if add:
            zg_arrive(dr, k - 1, t, c)
            value = value + zr[dr, k - 1, t, :, a:b].astype(F32)
        zs[dr, k, t, :, a:b] = value.astype(BF)
        src, dst = zg_refs(dr, k, t, c)
        send(src, dst, zg_s.at[dr, k, t, c], zg_r.at[dr, k, t, c], z_to[dr])

    steps = width // tile // 2
    for c in (0, 1):
        lax.fori_loop(c * steps, (c + 1) * steps, grad_tile, 0)
        for t in range(3):
            zg(c, 0, t, c, False)
        for t in range(3):
            zg(1 - c, 1, t, c, False)

    def part_tile(i, carry):
        p = jnp.dot(
            pair[pl.ds(pl.multiple_of(i * 128, 128), 128), :],
            w_all[0:2].reshape(256, width),
            preferred_element_type=F32,
        )
        part[pl.ds(i * 2, 2)] = p.reshape(2, 64, width)
        return carry

    lax.fori_loop(0, 4, part_tile, 0)

    for rel in (1, 0):
        for dr in (0, 1):
            ps0[dr, rel] = part[dpx(rel, 2), dr * 32 : (dr + 1) * 32].astype(BF)
            send(ps0.at[dr, rel], pr0.at[dr, rel], p0_s.at[dr, rel], p0_r.at[dr, rel], x_to[dr])

    def p1_send(dr, rel, h):
        send(ps1.at[dr, rel, h], pr1.at[dr, rel, h], p1_s.at[dr, rel, h], p1_r.at[dr, rel, h], x_to[dr])

    for rel in (1, 0):
        for dr in (0, 1):
            h = 1 - dr
            ps1[dr, rel, h] = part[dpx(rel, 1 if dr == 0 else -1), h * 32 : (h + 1) * 32].astype(BF)
            p1_send(dr, rel, h)

    def p1_step(rel):
        for dr in (0, 1):
            arrive(pr0.at[dr, rel], p0_s.at[dr, rel], p0_r.at[dr, rel], x_to[1 - dr])
            h = dr
            mine = part[dpx(rel, 1 if dr == 0 else -1), h * 32 : (h + 1) * 32]
            ps1[dr, rel, h] = (mine + pr0[dr, rel].astype(F32)).astype(BF)
            p1_send(dr, rel, h)

    def p2_sum(rel, h):
        for dr in (0, 1):
            arrive(
                pr1.at[dr, rel, h], p1_s.at[dr, rel, h], p1_r.at[dr, rel, h], x_to[1 - dr]
            )
        return (
            part[dpx(rel, 0), h * 32 : (h + 1) * 32]
            + pr1[0, rel, h].astype(F32)
            + pr1[1, rel, h].astype(F32)
        )

    def zg_all(k, c):
        for dr in (0, 1):
            for t in range(3):
                zg(dr, k, t, dr if c is None else c, True)

    zg_all(1, None)
    p1_step(1)
    zg_all(2, 1)
    p1_step(0)
    zg_all(2, 0)
    zg_all(3, 1)
    for h in (0, 1):
        ys[h] = p2_sum(1, h).astype(BF)
        send(ys.at[h], yr.at[h], yb_s.at[h], yb_r.at[h], y_to)
    zg_all(3, 0)

    def final(t, c):
        a, b = c * half, (c + 1) * half
        for dr in (0, 1):
            zg_arrive(dr, 3, t, c)
        total = grad[t, s, :, a:b]
        for dr in (0, 1):
            total = total + zr[dr, 3, t, :, a:b].astype(F32)
        fg[t][dp, :, a:b] = total.astype(BF)

    order = [(0, 1), (1, 1), (2, 1), (0, 0), (1, 0), (2, 0)]

    def fg_piece(p, rel, k):
        t, c = order[p]
        return fg[t].at[dpx(rel, k), :, pl.ds(c * half, half)]

    def fg_send_x(p, rel):
        for dr in (0, 1):
            ref = fg_piece(p, rel, 0)
            send(ref, ref, xg_s.at[dr, rel, p], xg_r.at[dr, rel, p], x_to[dr])

    def fg_own(p):
        final(*order[p])
        ref = fg_piece(p, 0, 0)
        if p < 5:
            send(ref, ref, yg_s.at[p], yg_r.at[p], y_to)
            fg_send_x(p, 0)
        else:
            for i, to in enumerate(all_to):
                send(ref, ref, dg_s.at[i], dg_r.at[i], to)

    def fg_y(p):
        arrive(fg_piece(p, 1, 0), yg_s.at[p], yg_r.at[p], y_to)
        fg_send_x(p, 1)

    def fg_x(p, rel):
        for dr in (0, 1):
            ref = fg_piece(p, rel, -1 if dr == 0 else 1)
            arrive(ref, xg_s.at[dr, rel, p], xg_r.at[dr, rel, p], x_to[1 - dr])
            if p % 2 == dr:
                send(ref, ref, xh_s.at[rel, p], xh_r.at[rel, p], x_to[dr])

    for p in (0, 1, 2):
        fg_own(p)
    for h in (0, 1):
        mine = p2_sum(0, h)
        arrive(yr.at[h], yb_s.at[h], yb_r.at[h], y_to)
        total = mine + yr[h].astype(F32)
        bs[h * 4 : (h + 1) * 4] = total.reshape(4, CAP, width).astype(BF)
    for i in range(1, 8):
        send(bs.at[flip(FLIPS[i])], br.at[e], cb_s.at[i], cb_r.at[i], c_to[i])
    br[e] = bs[e]
    for p in (0, 1, 2):
        fg_y(p)
    for p in (3, 4, 5):
        fg_own(p)
    for rel in (0, 1):
        for p in (0, 1, 2):
            fg_x(p, rel)
    for p in (3, 4):
        fg_y(p)
    for i in range(1, 8):
        arrive(br.at[flip(FLIPS[i])], cb_s.at[i], cb_r.at[i], c_to[i])
    gi_ref[...] = lax.dot_general(
        picker,
        br[...].astype(F32).reshape(64, width).astype(BF),
        (((0,), (0,)), ((), ())),
        preferred_element_type=F32,
    ).astype(BF)
    for rel in (0, 1):
        for p in (3, 4):
            fg_x(p, rel)
    for rel in (0, 1):
        for p in range(5):
            arrive(fg_piece(p, rel, 2), xh_s.at[rel, p], xh_r.at[rel, p], x_to[1 - p % 2])
    for i, (rel, k) in enumerate(ALL):
        arrive(fg_piece(5, rel, -k), dg_s.at[i], dg_r.at[i], (dpx(rel, -k), ex))
    for c in sends:
        c.wait_send()


def finish(gi, gg, gu, gd, gi_out, gg_out, gu_out, gd_out, turned, sem):
    outs = [pltpu.make_async_copy(gi, gi_out, sem.at[0]), pltpu.make_async_copy(gd, gd_out, sem.at[1])]
    for c in outs:
        c.start()
    for i, (src, dst) in enumerate(((gg, gg_out), (gu, gu_out))):
        turned[i] = src[...].T
        c = pltpu.make_async_copy(turned.at[i], dst, sem.at[2 + i])
        c.start()
        outs.append(c)
    for c in outs:
        c.wait()


def local(tokens, cotangent, expert_ids, gate_probs, gate_weight, up_weight, down_weight):
    rows, width = tokens.shape
    hid = down_weight.shape[1]
    v = pl.BlockSpec(memory_space=pltpu.VMEM)
    a = pl.BlockSpec(memory_space=pl.ANY)
    vm = pltpu.VMEM
    grad = jax.ShapeDtypeStruct((8, 16, width), BF)
    grad_input, *grads = pl.pallas_call(
        kernel,
        out_shape=(
            jax.ShapeDtypeStruct((rows, width), BF),
            grad,
            grad,
            grad,
        ),
        in_specs=[a] * 7,
        out_specs=(v, v, v, v),
        scratch_shapes=[
            vm((8, 128), jnp.int32),
            vm((8, 128), F32),
            vm((rows, width), BF),
            vm((rows, width), BF),
            vm((width, hid), BF),
            vm((width, hid), BF),
            vm((8, 16, width), BF),
            vm((8, 8, 16, width), BF),
            vm((3, 8, 16, width), BF),
            vm((384, 1024), BF),
            vm((512, 256), BF),
            vm((3, 8, 16, width), F32),
            vm((8, 64, width), F32),
            vm((2, 4, 3, 16, width), BF),
            vm((2, 4, 3, 16, width), BF),
            vm((2, 2, 32, width), BF),
            vm((2, 2, 32, width), BF),
            vm((2, 2, 2, 32, width), BF),
            vm((2, 2, 2, 32, width), BF),
            vm((2, 32, width), BF),
            vm((2, 32, width), BF),
            vm((8, 8, width), BF),
            vm((8, 8, width), BF),
            DMA((7,)),
            DMA((2, 4, 3)),
            DMA((2, 4, 3)),
            DMA((8,)),
            DMA((8,)),
            DMA((6,)),
            DMA((6,)),
            DMA((2, 2, 6)),
            DMA((2, 2, 6)),
            DMA((2, 6)),
            DMA((2, 6)),
            DMA((2, 3)),
            DMA((2, 3)),
            DMA((2, 4, 3, 2)),
            DMA((2, 4, 3, 2)),
            DMA((2, 2)),
            DMA((2, 2)),
            DMA((2, 2, 2)),
            DMA((2, 2, 2)),
            DMA((2,)),
            DMA((2,)),
            DMA((8,)),
            DMA((8,)),
            DMA((5,)),
            DMA((5,)),
            DMA((2, 2, 5)),
            DMA((2, 2, 5)),
            DMA((2, 5)),
            DMA((2, 5)),
            DMA((7,)),
            DMA((7,)),
        ],
        compiler_params=pltpu.CompilerParams(
            collective_id=0, has_side_effects=True, vmem_limit_bytes=40 * 1024 * 1024
        ),
    )(
        *[
            pltpu.with_memory_space_constraint(i, pltpu.MemorySpace.HBM)
            for i in (expert_ids.T, gate_probs.T, tokens, cotangent, gate_weight, up_weight, down_weight)
        ],
    )
    flat = jax.ShapeDtypeStruct((hid, width), BF)
    tall = jax.ShapeDtypeStruct((width, hid), BF)
    grads = [g.reshape(hid, width) for g in grads]
    grad_input, gate, up, down = pl.pallas_call(
        finish,
        out_shape=(flat, tall, tall, flat),
        in_specs=[v] * 4,
        out_specs=(a, a, a, a),
        scratch_shapes=[vm((2, width, hid), BF), DMA((4,))],
        compiler_params=pltpu.CompilerParams(vmem_limit_bytes=40 * 1024 * 1024),
    )(grad_input, *grads)
    return (grad_input, gate[None], up[None], down[None])


def solution(mesh):
    tok = P(("dp", "expert"), None)
    wgt = P("expert", None, None)
    return jax.shard_map(
        local,
        mesh=mesh,
        in_specs=(tok, tok, tok, tok, wgt, wgt, wgt),
        out_specs=(tok, wgt, wgt, wgt),
        check_vma=False,
    )
```

```python
import jax
import jax.numpy as jnp
from jax import lax
from jax.experimental import pallas as pl
from jax.experimental.pallas import tpu as pltpu
from jax.sharding import PartitionSpec as P

SLICES = 8
CAP = 8
XS = 4
BF = jnp.bfloat16
F32 = jnp.float32
MESH = pl.DeviceIdType.MESH
DMA = pltpu.SemaphoreType.DMA
ALL = [(0, 1), (0, -1), (1, 0), (0, 2), (1, 1), (1, -1), (1, 2)]
FLIPS = [(fz, fy, fc) for fz in (0, 1) for fy in (0, 1) for fc in (0, 1)]


def kernel(
    ids_hbm,
    probs_hbm,
    tok_hbm,
    cot_hbm,
    gate_hbm,
    up_hbm,
    down_hbm,
    gi_ref,
    gg_ref,
    gu_ref,
    gd_ref,
    ids_ref,
    probs_ref,
    tok,
    cot,
    gate,
    up,
    msg,
    x_all,
    w_all,
    lt,
    pair,
    grad,
    part,
    zs,
    zr,
    ps0,
    pr0,
    ps1,
    pr1,
    ys,
    yr,
    bs,
    br,
    load_sem,
    za_s,
    za_r,
    ca_s,
    ca_r,
    ya_s,
    ya_r,
    xa_s,
    xa_r,
    xb_s,
    xb_r,
    yx_s,
    yx_r,
    zg_s,
    zg_r,
    p0_s,
    p0_r,
    p1_s,
    p1_r,
    yb_s,
    yb_r,
    cb_s,
    cb_r,
    yg_s,
    yg_r,
    xg_s,
    xg_r,
    xh_s,
    xh_r,
    dg_s,
    dg_r,
    yq_s,
    yq_r,
):
    fg = (gg_ref, gu_ref, gd_ref)
    width = tok.shape[1]
    half = width // 2
    dp = lax.axis_index("dp")
    ex = lax.axis_index("expert")
    s = ex // 8
    e = ex % 8
    zb, yl, co = e // 4, (e // 2) % 2, e % 2
    x, yh = dp % XS, dp // XS
    oyh = 1 - yh

    def ring(k):
        return (s + k + 8) % 8

    def flip(f):
        fz, fy, fc = f
        return ((zb + fz) % 2) * 4 + ((yl + fy) % 2) * 2 + (co + fc) % 2

    def group(j):
        return ((zb + j // 2) % 2) * 2 + (yl + j % 2) % 2

    def dpx(rel, k):
        return (oyh if rel else yh) * XS + (x + k + XS) % XS

    z_to = [(dp, ring(1) * 8 + e), (dp, ring(-1) * 8 + e)]
    x_to = [(dpx(0, 1), ex), (dpx(0, -1), ex)]
    y_to = (dpx(1, 0), ex)
    all_to = [(dpx(rel, k), ex) for rel, k in ALL]
    far_to = [(dpx(rel, k), ex) for rel, k in ALL[3:]]
    c_to = [(dp, s * 8 + flip(f)) for f in FLIPS]
    sends = []

    def send(src, dst, ssem, rsem, to):
        c = pltpu.make_async_remote_copy(
            src_ref=src, dst_ref=dst, send_sem=ssem, recv_sem=rsem, device_id=to, device_id_type=MESH
        )
        c.start()
        sends.append(c)

    def arrive(dst, ssem, rsem, frm):
        pltpu.make_async_remote_copy(
            src_ref=dst, dst_ref=dst, send_sem=ssem, recv_sem=rsem, device_id=frm, device_id_type=MESH
        ).wait_recv()

    barrier = pltpu.get_barrier_semaphore()
    partners = z_to + x_to + [y_to] + c_to[1:] + far_to
    for to in partners:
        pl.semaphore_signal(barrier, inc=1, device_id=to, device_id_type=MESH)

    piece = down_hbm.at[0, pl.ds(pl.multiple_of(dp * 16, 16), 16)]
    loads = [
        pltpu.make_async_copy(a, b, load_sem.at[i])
        for i, (a, b) in enumerate(
            [(piece, w_all.at[2, s]), (tok_hbm, tok), (cot_hbm, cot), (gate_hbm.at[0], gate),
             (up_hbm.at[0], up), (ids_hbm, ids_ref), (probs_hbm, probs_ref)]
        )
    ]
    for i in (5, 6, 0, 1, 2, 3, 4):
        loads[i].start()

    loads[5].wait()
    loads[6].wait()
    ids = ids_ref[...]
    probs = probs_ref[...]
    want = lax.broadcasted_iota(jnp.int32, (64, 128), 0) // CAP
    slot = (lax.broadcasted_iota(jnp.int32, (64, 128), 0) % CAP).astype(F32)
    hit = jnp.zeros((64, 128), F32)
    chosen = jnp.zeros((64, 128), F32)
    for k in range(ids.shape[0]):
        m = ids[k : k + 1, :] == want
        hit = hit + jnp.where(m, 1.0, 0.0)
        chosen = chosen + jnp.where(m, probs[k : k + 1, :], 0.0)
    before = jnp.where(
        lax.broadcasted_iota(jnp.int32, (128, 128), 0) < lax.broadcasted_iota(jnp.int32, (128, 128), 1),
        1.0,
        0.0,
    ).astype(BF)
    rank = jnp.dot(hit.astype(BF), before, preferred_element_type=F32)
    placed = jnp.where((hit == 1.0) & (rank == slot), 1.0, 0.0)
    picker = placed.astype(BF)
    prob = jnp.sum(placed * chosen, axis=1, keepdims=True)

    pl.semaphore_wait(barrier, len(partners))

    def w_send(dr, k, t):
        c = ring(-k if dr == 0 else k)
        ref = w_all.at[t, c] if k < 3 else w_all.at[t, c, :, pl.ds(dr * half, half)]
        send(ref, ref, za_s.at[dr, k, t], za_r.at[dr, k, t], z_to[dr])

    def w_arrive(k, t):
        for dr in (0, 1):
            c = ring(-1 - k if dr == 0 else 1 + k)
            ref = w_all.at[t, c] if k < 3 else w_all.at[t, c, :, pl.ds(dr * half, half)]
            arrive(ref, za_s.at[dr, k, t], za_r.at[dr, k, t], z_to[1 - dr])
            if k < 3:
                w_send(dr, k + 1, t)

    loads[0].wait()
    for dr in (0, 1):
        w_send(dr, 0, 2)

    loads[1].wait()
    rows_in = jnp.dot(picker, tok[...], preferred_element_type=F32)
    loads[2].wait()
    rows_cot = prob * jnp.dot(picker, cot[...], preferred_element_type=F32)
    msg[...] = jnp.concatenate(
        [rows_in.reshape(8, CAP, width), rows_cot.reshape(8, CAP, width)], axis=1
    ).astype(BF)
    for i in range(1, 8):
        send(msg.at[flip(FLIPS[i])], x_all.at[dp, e], ca_s.at[i], ca_r.at[i], c_to[i])
    x_all[dp, e] = msg[e]

    def unit(d, u):
        first, n = [(e, 1), (flip((0, 0, 1)), 1), (group(1) * 2, 2), (group(2) * 2, 2),
                    (flip((1, 1, 0)), 1), (flip((1, 1, 1)), 1)][u]
        return x_all.at[d, pl.ds(first, n)]

    def xa_send(rel, u):
        for dr in (0, 1):
            ref = unit(dpx(rel, 0), u)
            send(ref, ref, xa_s.at[dr, rel, u], xa_r.at[dr, rel, u], x_to[dr])

    def own(u):
        for i in [(), (1,), (2, 3), (4, 5), (6,), (7,)][u]:
            arrive(x_all.at[dp, flip(FLIPS[i])], ca_s.at[i], ca_r.at[i], c_to[i])
        xa_send(0, u)
        ref = unit(dp, u)
        send(ref, ref, ya_s.at[u], ya_r.at[u], y_to)

    def yx_send(u, i, k):
        ref = unit(dpx(0, k), u)
        send(ref, ref, yx_s.at[u, i], yx_r.at[u, i], y_to)

    def y_in(u):
        arrive(unit(dpx(1, 0), u), ya_s.at[u], ya_r.at[u], y_to)
        if u >= 2:
            xa_send(1, u)

    def x_in(dr, rel, u):
        k = -1 if dr == 0 else 1
        ref = unit(dpx(rel, k), u)
        arrive(ref, xa_s.at[dr, rel, u], xa_r.at[dr, rel, u], x_to[1 - dr])
        if u % 2 == dr:
            send(ref, ref, xb_s.at[rel, u], xb_r.at[rel, u], x_to[dr])
        if u < 2:
            yx_send(u, dr, k)

    def far_in(rel, u):
        dr = u % 2
        arrive(unit(dpx(rel, 2), u), xb_s.at[rel, u], xb_r.at[rel, u], x_to[1 - dr])
        if u < 2:
            yx_send(u, 2, 2)

    def yx_in(i, k):
        for u in (0, 1):
            arrive(unit(dpx(1, k), u), yx_s.at[u, i], yx_r.at[u, i], y_to)

    own(0)

    row = lax.broadcasted_iota(jnp.int32, (16, 128), 0)
    lane = lax.broadcasted_iota(jnp.int32, (16, 128), 1)
    sel = jnp.where(lane == row + dp * 16, 1.0, 0.0).astype(BF)
    for t, ref in ((0, gate), (1, up)):
        loads[3 + t].wait()
        w_all[t, s] = lax.dot_general(
            sel, ref[...], (((1,), (1,)), ((), ())), preferred_element_type=F32
        ).astype(BF)
        for dr in (0, 1):
            w_send(dr, 0, t)
        if t == 0:
            own(1)

    own(2)
    own(3)
    x_in(0, 0, 0)
    w_arrive(0, 2)
    x_in(1, 0, 1)
    x_in(1, 0, 0)
    x_in(0, 0, 1)
    own(4)
    own(5)
    w_arrive(0, 0)
    far_in(0, 0)
    far_in(0, 1)
    w_arrive(0, 1)
    y_in(2)
    x_in(0, 0, 2)
    w_arrive(1, 2)
    y_in(3)
    x_in(1, 0, 3)
    w_arrive(1, 0)
    y_in(4)
    y_in(5)
    x_in(0, 0, 4)
    x_in(1, 0, 5)
    w_arrive(1, 1)
    w_arrive(2, 2)
    x_in(0, 1, 2)
    w_arrive(2, 0)
    x_in(1, 1, 3)
    w_arrive(2, 1)
    x_in(0, 1, 4)
    x_in(1, 1, 5)
    for t in (2, 0, 1):
        w_arrive(3, t)

    def compute(k):
        d = (dpx(0, k), dpx(1, k))
        rows = jnp.concatenate([x_all[i].reshape(128, width) for i in d], axis=0)
        first = lax.dot_general(
            rows, w_all[...].reshape(384, width), (((1,), (1,)), ((), ())), preferred_element_type=F32
        ).reshape(16, 2, CAP, 384)
        pre = first[:, 0, :, 0:128]
        upward = first[:, 0, :, 128:256]
        dhidden = first[:, 1, :, 256:384]
        sigmoid = jax.nn.sigmoid(pre)
        swish = pre * sigmoid
        slope = sigmoid * (1.0 + pre * (1.0 - sigmoid))
        active = swish * upward
        dgate = dhidden * upward * slope
        dupward = dhidden * swish
        zero = jnp.zeros_like(active)
        top = jnp.concatenate([dgate, dupward, zero], axis=2)
        low = jnp.concatenate([zero, zero, active], axis=2)
        both = jnp.concatenate([top[:, None], low[:, None]], axis=1).reshape(256, 384).astype(BF).T
        pairs = top.reshape(128, 384)[:, :256].astype(BF)
        for i in (0, 1):
            lt[:, pl.ds(pl.multiple_of(d[i] * 128, 128), 128)] = both[:, i * 128 : (i + 1) * 128]
            pair[pl.ds(pl.multiple_of(d[i] * 64, 64), 64), :] = pairs[i * 64 : (i + 1) * 64]

    y_in(0)
    y_in(1)
    compute(0)
    for dr in (0, 1):
        for rel in (0, 1):
            for u in (2, 3, 4, 5):
                if u % 2 != dr:
                    x_in(dr, rel, u)
        yx_in(dr, -1 if dr == 0 else 1)
        compute(-1 if dr == 0 else 1)
    for rel in (0, 1):
        for u in (2, 3, 4, 5):
            far_in(rel, u)
    yx_in(2, 2)
    compute(2)

    tile = 512

    def grad_tile(n, carry):
        cols = pl.ds(pl.multiple_of(n * tile, tile), tile)
        g = jnp.dot(lt[...], x_all[:, :, :, cols].reshape(1024, tile), preferred_element_type=F32)
        grad[:, :, :, cols] = g.reshape(3, 8, 16, tile)
        return carry

    def zg_refs(dr, k, t, c):
        cols = pl.ds(c * half, half)
        return zs.at[dr, k, t, :, cols], zr.at[dr, k, t, :, cols]

    def zg_arrive(dr, k, t, c):
        arrive(zg_refs(dr, k, t, c)[1], zg_s.at[dr, k, t, c], zg_r.at[dr, k, t, c], z_to[1 - dr])

    def zg(dr, k, t, c, add):
        a, b = c * half, (c + 1) * half
        value = grad[t, ring((4 - k) if dr == 0 else (k - 4)), :, a:b]
        if add:
            zg_arrive(dr, k - 1, t, c)
            value = value + zr[dr, k - 1, t, :, a:b].astype(F32)
        zs[dr, k, t, :, a:b] = value.astype(BF)
        src, dst = zg_refs(dr, k, t, c)
        send(src, dst, zg_s.at[dr, k, t, c], zg_r.at[dr, k, t, c], z_to[dr])

    steps = width // tile // 2
    for c in (0, 1):
        lax.fori_loop(c * steps, (c + 1) * steps, grad_tile, 0, unroll=True)
        for t in range(3):
            zg(c, 0, t, c, False)
        for t in range(3):
            zg(1 - c, 1, t, c, False)

    def part_tile(i, carry):
        p = jnp.dot(
            pair[pl.ds(pl.multiple_of(i * 128, 128), 128), :],
            w_all[0:2].reshape(256, width),
            preferred_element_type=F32,
        )
        part[pl.ds(i * 2, 2)] = p.reshape(2, 64, width)
        return carry

    lax.fori_loop(0, 4, part_tile, 0, unroll=True)

    for rel in (1, 0):
        for dr in (0, 1):
            ps0[dr, rel] = part[dpx(rel, 2), dr * 32 : (dr + 1) * 32].astype(BF)
            send(ps0.at[dr, rel], pr0.at[dr, rel], p0_s.at[dr, rel], p0_r.at[dr, rel], x_to[dr])

    def p1_send(dr, rel, h):
        send(ps1.at[dr, rel, h], pr1.at[dr, rel, h], p1_s.at[dr, rel, h], p1_r.at[dr, rel, h], x_to[dr])

    for rel in (1, 0):
        for dr in (0, 1):
            h = 1 - dr
            ps1[dr, rel, h] = part[dpx(rel, 1 if dr == 0 else -1), h * 32 : (h + 1) * 32].astype(BF)
            p1_send(dr, rel, h)

    def p1_step(rel):
        for dr in (0, 1):
            arrive(pr0.at[dr, rel], p0_s.at[dr, rel], p0_r.at[dr, rel], x_to[1 - dr])
            h = dr
            mine = part[dpx(rel, 1 if dr == 0 else -1), h * 32 : (h + 1) * 32]
            ps1[dr, rel, h] = (mine + pr0[dr, rel].astype(F32)).astype(BF)
            p1_send(dr, rel, h)

    def p2_sum(rel, h):
        for dr in (0, 1):
            arrive(
                pr1.at[dr, rel, h], p1_s.at[dr, rel, h], p1_r.at[dr, rel, h], x_to[1 - dr]
            )
        return (
            part[dpx(rel, 0), h * 32 : (h + 1) * 32]
            + pr1[0, rel, h].astype(F32)
            + pr1[1, rel, h].astype(F32)
        )

    def zg_all(k, c):
        for dr in (0, 1):
            for t in range(3):
                zg(dr, k, t, dr if c is None else c, True)

    zg_all(1, None)
    p1_step(1)
    zg_all(2, 1)
    p1_step(0)
    zg_all(2, 0)
    zg_all(3, 1)
    for h in (0, 1):
        ys[h] = p2_sum(1, h).astype(BF)
        send(ys.at[h], yr.at[h], yb_s.at[h], yb_r.at[h], y_to)
    zg_all(3, 0)

    def final(t, c):
        a, b = c * half, (c + 1) * half
        for dr in (0, 1):
            zg_arrive(dr, 3, t, c)
        total = grad[t, s, :, a:b]
        for dr in (0, 1):
            total = total + zr[dr, 3, t, :, a:b].astype(F32)
        fg[t][dp, :, a:b] = total.astype(BF)

    order = [(0, 1), (1, 1), (2, 1), (0, 0), (1, 0), (2, 0)]

    def fg_piece(p, rel, k):
        t, c = order[p]
        return fg[t].at[dpx(rel, k), :, pl.ds(c * half, half)]

    def fg_send_x(p, rel):
        for dr in (0, 1):
            ref = fg_piece(p, rel, 0)
            send(ref, ref, xg_s.at[dr, rel, p], xg_r.at[dr, rel, p], x_to[dr])

    def fg_own(p):
        final(*order[p])
        ref = fg_piece(p, 0, 0)
        if p < 5:
            send(ref, ref, yg_s.at[p], yg_r.at[p], y_to)
            fg_send_x(p, 0)
        else:
            for i, to in enumerate(all_to):
                send(ref, ref, dg_s.at[i], dg_r.at[i], to)

    def fg_y(p):
        arrive(fg_piece(p, 1, 0), yg_s.at[p], yg_r.at[p], y_to)
        if p >= 2:
            fg_send_x(p, 1)

    def fg_down(p, i, k):
        ref = fg_piece(p, 0, k)
        send(ref, ref, yq_s.at[p, i], yq_r.at[p, i], y_to)

    def fg_far(p, rel):
        arrive(fg_piece(p, rel, 2), xh_s.at[rel, p], xh_r.at[rel, p], x_to[1 - p % 2])
        if p < 2:
            fg_down(p, 2, 2)

    def fg_x(p, rel):
        for dr in (0, 1):
            ref = fg_piece(p, rel, -1 if dr == 0 else 1)
            arrive(ref, xg_s.at[dr, rel, p], xg_r.at[dr, rel, p], x_to[1 - dr])
            if p % 2 == dr:
                send(ref, ref, xh_s.at[rel, p], xh_r.at[rel, p], x_to[dr])
            if p < 2:
                fg_down(p, dr, -1 if dr == 0 else 1)

    for p in (0, 1, 2):
        fg_own(p)
    for h in (0, 1):
        mine = p2_sum(0, h)
        arrive(yr.at[h], yb_s.at[h], yb_r.at[h], y_to)
        total = mine + yr[h].astype(F32)
        bs[h * 4 : (h + 1) * 4] = total.reshape(4, CAP, width).astype(BF)
    for i in range(1, 8):
        send(bs.at[flip(FLIPS[i])], br.at[e], cb_s.at[i], cb_r.at[i], c_to[i])
    br[e] = bs[e]
    fg_x(0, 0)
    fg_x(1, 0)
    fg_y(2)
    fg_own(3)
    fg_far(0, 0)
    fg_far(1, 0)
    fg_own(4)
    fg_own(5)
    fg_x(2, 0)
    fg_x(2, 1)
    for p in (3, 4):
        fg_y(p)
    for i in range(1, 8):
        arrive(br.at[flip(FLIPS[i])], cb_s.at[i], cb_r.at[i], c_to[i])
    gi_ref[...] = lax.dot_general(
        picker,
        br[...].astype(F32).reshape(64, width).astype(BF),
        (((0,), (0,)), ((), ())),
        preferred_element_type=F32,
    ).astype(BF)
    for rel in (0, 1):
        for p in (3, 4):
            fg_x(p, rel)
    for rel in (0, 1):
        for p in (2, 3, 4):
            fg_far(p, rel)
    for p in (0, 1):
        fg_y(p)
        for i, k in enumerate((-1, 1, 2)):
            arrive(fg_piece(p, 1, k), yq_s.at[p, i], yq_r.at[p, i], y_to)
    for i, (rel, k) in enumerate(ALL):
        arrive(fg_piece(5, rel, -k), dg_s.at[i], dg_r.at[i], (dpx(rel, -k), ex))
    for c in sends:
        c.wait_send()


def finish(gi, gg, gu, gd, gi_out, gg_out, gu_out, gd_out, turned, sem):
    outs = [pltpu.make_async_copy(gi, gi_out, sem.at[0]), pltpu.make_async_copy(gd, gd_out, sem.at[1])]
    for c in outs:
        c.start()
    for i, (src, dst) in enumerate(((gg, gg_out), (gu, gu_out))):
        turned[i] = src[...].T
        c = pltpu.make_async_copy(turned.at[i], dst, sem.at[2 + i])
        c.start()
        outs.append(c)
    for c in outs:
        c.wait()


def local(tokens, cotangent, expert_ids, gate_probs, gate_weight, up_weight, down_weight):
    rows, width = tokens.shape
    hid = down_weight.shape[1]
    v = pl.BlockSpec(memory_space=pltpu.VMEM)
    a = pl.BlockSpec(memory_space=pl.ANY)
    vm = pltpu.VMEM
    grad = jax.ShapeDtypeStruct((8, 16, width), BF)
    grad_input, *grads = pl.pallas_call(
        kernel,
        out_shape=(
            jax.ShapeDtypeStruct((rows, width), BF),
            grad,
            grad,
            grad,
        ),
        in_specs=[a] * 7,
        out_specs=(v, v, v, v),
        scratch_shapes=[
            vm((8, 128), jnp.int32),
            vm((8, 128), F32),
            vm((rows, width), BF),
            vm((rows, width), BF),
            vm((width, hid), BF),
            vm((width, hid), BF),
            vm((8, 16, width), BF),
            vm((8, 8, 16, width), BF),
            vm((3, 8, 16, width), BF),
            vm((384, 1024), BF),
            vm((512, 256), BF),
            vm((3, 8, 16, width), F32),
            vm((8, 64, width), F32),
            vm((2, 4, 3, 16, width), BF),
            vm((2, 4, 3, 16, width), BF),
            vm((2, 2, 32, width), BF),
            vm((2, 2, 32, width), BF),
            vm((2, 2, 2, 32, width), BF),
            vm((2, 2, 2, 32, width), BF),
            vm((2, 32, width), BF),
            vm((2, 32, width), BF),
            vm((8, 8, width), BF),
            vm((8, 8, width), BF),
            DMA((7,)),
            DMA((2, 4, 3)),
            DMA((2, 4, 3)),
            DMA((8,)),
            DMA((8,)),
            DMA((6,)),
            DMA((6,)),
            DMA((2, 2, 6)),
            DMA((2, 2, 6)),
            DMA((2, 6)),
            DMA((2, 6)),
            DMA((2, 3)),
            DMA((2, 3)),
            DMA((2, 4, 3, 2)),
            DMA((2, 4, 3, 2)),
            DMA((2, 2)),
            DMA((2, 2)),
            DMA((2, 2, 2)),
            DMA((2, 2, 2)),
            DMA((2,)),
            DMA((2,)),
            DMA((8,)),
            DMA((8,)),
            DMA((5,)),
            DMA((5,)),
            DMA((2, 2, 5)),
            DMA((2, 2, 5)),
            DMA((2, 5)),
            DMA((2, 5)),
            DMA((7,)),
            DMA((7,)),
            DMA((2, 3)),
            DMA((2, 3)),
        ],
        compiler_params=pltpu.CompilerParams(
            collective_id=0, has_side_effects=True, vmem_limit_bytes=40 * 1024 * 1024
        ),
    )(
        *[
            pltpu.with_memory_space_constraint(i, pltpu.MemorySpace.HBM)
            for i in (expert_ids.T, gate_probs.T, tokens, cotangent, gate_weight, up_weight, down_weight)
        ],
    )
    flat = jax.ShapeDtypeStruct((hid, width), BF)
    tall = jax.ShapeDtypeStruct((width, hid), BF)
    grads = [g.reshape(hid, width) for g in grads]
    grad_input, gate, up, down = pl.pallas_call(
        finish,
        out_shape=(flat, tall, tall, flat),
        in_specs=[v] * 4,
        out_specs=(a, a, a, a),
        scratch_shapes=[vm((2, width, hid), BF), DMA((4,))],
        compiler_params=pltpu.CompilerParams(vmem_limit_bytes=40 * 1024 * 1024),
    )(grad_input, *grads)
    return (grad_input, gate[None], up[None], down[None])


def solution(mesh):
    tok = P(("dp", "expert"), None)
    wgt = P("expert", None, None)
    return jax.shard_map(
        local,
        mesh=mesh,
        in_specs=(tok, tok, tok, tok, wgt, wgt, wgt),
        out_specs=(tok, wgt, wgt, wgt),
        check_vma=False,
    )
```
